256 devices in a mesh: ep: 8 (over z), tp: 32 (over y, x, core).
Axes of the slice: x: 4, y: 4, z: 8, core: 2. Of those that a mesh axis runs over, the one named last changes fastest.
Arguments:
- tokens: bfloat16 [768, 3072], P('ep', 'tp'), may hold values from -6 to 6
- cotangent: bfloat16 [768, 3072], P('ep', 'tp'), may hold values from -6 to 6
- expert_ids: int32 [768, 2], P('ep'), may hold values from 0 to 7, all different within a row; in each aligned block of 96 rows (0 to 95, 96 to 191, ...) at most 40 rows name the same one
- combine_weights: float32 [768, 2], P('ep'), may hold values from 0.1 to 1
- w_gate: bfloat16 [8, 3072, 8192], P('ep', None, 'tp'), may hold values from -0.21875 to 0.21875
- w_up: bfloat16 [8, 3072, 8192], P('ep', None, 'tp'), may hold values from -0.109375 to 0.109375
- w_down: bfloat16 [8, 8192, 3072], P('ep', 'tp'), may hold values from -0.125 to 0.125
Outputs:
- mixed: bfloat16 [768, 3072], P('ep', 'tp')
- grad_tokens: bfloat16 [768, 3072], P('ep', 'tp')
- grad_combine: float32 [768, 2], P('ep')
- grad_gate: bfloat16 [8, 3072, 8192], P('ep', 'tp')
- grad_up: bfloat16 [8, 3072, 8192], P('ep', 'tp')
- grad_down: bfloat16 [8, 8192, 3072], P('ep', None, 'tp')
The draws below stay inside these ranges and needn't reach their ends.
Inputs may be any that keep to these rules, and one draw needn't show every extreme that they name: `expert_ids`: each row names 2 different experts. Among the 96 rows of one index of ep, no expert is named more than 40 times, and in some such blocks one expert is named exactly 40 times.
All inputs are finite; a program needn't handle non-finite values.
Results may differ from the reference program's by a relative error of at most 0.019.
Values may be sent and summed in bfloat16 or wider, within the bound.
A program may use at most 64 MiB of HBM per device.

```python
import math
import jax
import jax.numpy as jnp
import numpy as np
from jax import lax

D = 3072
FF = 8192
TOP = 2
TOK_EP = 96
EXPERTS = 8
CAP = 40
TOKENS = 768
N_EP = 8
N_TP = 32


def with_spikes(drawn, stream_key, source, target, parts, factor):
    def block_of(axis_at):
        return (jnp.arange(drawn.shape[axis_at]) // (drawn.shape[axis_at] // parts)).reshape((-1,) + (1,) * (drawn.ndim - 1 - axis_at))

    first = jax.random.permutation(stream_key, parts)[block_of(target)]
    other_side = (block_of(target) + parts // 2) % parts
    return jnp.where((block_of(source) == first) | (block_of(source) == other_side), factor * drawn, drawn)


def level_of(stream_key, shape, shards, least, largest):
    def one(position, parts):
        draws = jax.random.uniform(jax.random.fold_in(jax.random.fold_in(stream_key, 6), position), (parts,), jnp.float32, least / len(shards), largest / len(shards))
        return jnp.repeat(jnp.exp(draws), shape[position] // parts).reshape((-1,) + (1,) * (len(shape) - position - 1))

    loudness = one(*shards[0])
    for cut in shards[1:]:
        loudness = loudness * one(*cut)
    return loudness


def assign_block(key, own, number, rows, amount, top, most, skew):
    ranking = jax.random.permutation(key, amount)
    packed, usual = shares(amount, rows * top, most, skew, True), shares(amount, rows * top, most, skew, False)
    places = jnp.arange(amount)

    def named(tallies, rotation):
        used = int((tallies > 0).sum())
        fixed = max(1, used // 4)
        passed = fixed + (places - fixed + rotation * (used - fixed)) % max(1, amount - fixed)
        return jnp.zeros((amount,), jnp.int32).at[ranking[jnp.where(places < fixed, places, passed)]].set(jnp.asarray(tallies, jnp.int32))

    tallies = jnp.where(number % 4 == 0, named(packed, number // 4), named(usual, number - number // 4 - 1))
    mixed = jax.random.permutation(jax.random.fold_in(own, 3), amount)
    giver, receiver = mixed[0:amount // 2 * 2:2], mixed[1:amount // 2 * 2:2]
    margin = jnp.minimum(tallies[giver] - 1, most - tallies[receiver]) // 2
    margin = jnp.where((giver == ranking[0]) | (receiver == ranking[0]) | (tallies[receiver] == 0), 0, jnp.maximum(margin, 0))
    passed = jax.random.randint(jax.random.fold_in(own, 4), (amount // 2,), 0, 1 << 20) % (margin + 1)
    tallies = tallies.at[giver].add(-passed).at[receiver].add(passed)
    members = jnp.searchsorted(jnp.cumsum(tallies), jnp.arange(rows * top), side="right").astype(jnp.int32)
    grid = members.reshape(top, rows).T
    grid = grid[jax.random.permutation(jax.random.fold_in(own, 1), rows)]
    rotation = jax.random.randint(jax.random.fold_in(own, 2), (rows, 1), 0, top)
    return jnp.take_along_axis(grid, (jnp.arange(top)[None, :] + rotation) % top, axis=1)


def shares(count, total, bound, lean, full):
    portions = [(1 << 20) // math.isqrt(standing ** lean) + 1 for standing in range(1, count + 1)]
    largest = bound if full else min(bound, max(-(-total // count), total * portions[0] // sum(portions)))
    least = 1 if total - largest >= count - 1 else 0
    given, spare = [largest] + [least] * (count - 1), total - largest - least * (count - 1)
    while spare > 0:
        candidates = [i for i in range(1, count) if given[i] < largest] or [i for i in range(1, count) if given[i] < bound]
        mass, left = sum([portions[i] for i in candidates]), spare
        for i in candidates:
            extra = min(bound - given[i], max(1, left * portions[i] // mass), spare)
            given[i] = given[i] + extra
            spare = spare - extra
    return np.array(given)


def noise(key, extent, scale, limit, cuts=(), held_as=jnp.bfloat16):
    result = scale * jax.random.normal(key, extent, jnp.float32)
    if cuts:
        result = result * level_of(key, extent, cuts, -0.22, 0.18)
    return jnp.clip(result, -limit, limit).astype(held_as)


def heavy_noise(own_key, dims, spread, bound, shards, heavy, kind=jnp.bfloat16):
    values = spread * jax.random.normal(own_key, dims, jnp.float32)
    if shards:
        values = values * level_of(own_key, dims, shards, -0.22, 0.18)
    return jnp.clip(with_spikes(values, jax.random.fold_in(own_key, 3), *heavy), -bound, bound).astype(kind)


def setup_inputs(seed: int = 0) -> dict:
    key_of = jax.random.split(jax.random.key(seed), 8)
    tokens = noise(key_of[0], (TOKENS, D), 1.0, 6.0, ((0, 8), (1, 32)))
    cotangent = noise(key_of[1], (TOKENS, D), 1.0, 6.0, ((0, 8), (1, 32)))
    expert_ids_keys = jax.random.split(jax.random.fold_in(key_of[2], 1), TOKENS // TOK_EP)
    expert_ids_turns = jax.random.permutation(jax.random.fold_in(key_of[2], 3), TOKENS // TOK_EP)
    expert_ids = jax.vmap(lambda own, number: assign_block(jax.random.fold_in(key_of[2], 2), own, number, TOK_EP, N_EP, TOP, CAP, 2))(expert_ids_keys, expert_ids_turns).reshape((TOKENS, TOP))
    combine_weights = jnp.clip(jnp.exp(math.log(1.0) - 2.3025851 * jax.random.uniform(key_of[3], (TOKENS, TOP), jnp.float32) ** level_of(key_of[3], (TOKENS, TOP), ((0, 8),), -0.2, 0.2)), 0.1, 1.0)
    w_gate = heavy_noise(key_of[4], (EXPERTS, D, FF), D ** -0.5, 0.21875, ((0, 8), (2, 32)), (2, 1, 32, 2.75))
    w_up = noise(key_of[5], (EXPERTS, D, FF), D ** -0.5, 0.109375, ((0, 8), (2, 32)))
    w_down = heavy_noise(key_of[6], (EXPERTS, FF, D), FF ** -0.5, 0.125, ((0, 8), (1, 32)), (1, 2, 32, 2.75))
    return {"tokens": tokens, "cotangent": cotangent, "expert_ids": expert_ids, "combine_weights": combine_weights, "w_gate": w_gate, "w_up": w_up, "w_down": w_down}


def silu_parts(gate_pre):
    sigma = jax.nn.sigmoid(gate_pre)
    return gate_pre * sigma, sigma * (1.0 + gate_pre * (1.0 - sigma))


def slot_rows(expert_ids):
    groups = expert_ids.reshape(N_EP, TOK_EP * TOP)
    onehot = (groups[:, :, None] == jnp.arange(N_EP, dtype=jnp.int32)[None, None, :]).astype(jnp.int32)
    before = jnp.cumsum(onehot, axis=1) - onehot
    rank = jnp.sum(before * onehot, axis=2)
    source = jnp.arange(N_EP, dtype=jnp.int32)[:, None]
    return (source * CAP + rank).reshape(-1).astype(jnp.int32)


def rounded_blocks(pairs, rows):
    width = FF // N_TP

    def step(total, index):
        start = index * width
        part = jnp.zeros((rows, D), jnp.float32)
        for left, right in pairs:
            left_block = lax.dynamic_slice_in_dim(left, start, width, 1)
            right_block = lax.dynamic_slice_in_dim(right, start, width, 0)
            part = part + jnp.dot(left_block, right_block, preferred_element_type=jnp.float32)
        rounded = lax.optimization_barrier(part.astype(jnp.bfloat16))
        return total + rounded.astype(jnp.float32), None

    total, _ = lax.scan(step, jnp.zeros((rows, D), jnp.float32), jnp.arange(N_TP, dtype=jnp.int32))
    return total.astype(jnp.bfloat16)


def reference(tokens, cotangent, expert_ids, combine_weights, w_gate, w_up, w_down):
    flat_ids = expert_ids.reshape(-1)
    rows = slot_rows(expert_ids)
    owner = jnp.repeat(jnp.arange(TOKENS, dtype=jnp.int32), TOP)
    weight_flat = combine_weights.reshape(-1)
    buffer_rows = N_EP * CAP
    x_buffer = jnp.zeros((N_EP, buffer_rows, D), jnp.bfloat16).at[flat_ids, rows].set(tokens[owner])
    grad_out = (weight_flat[:, None] * cotangent[owner].astype(jnp.float32)).astype(jnp.bfloat16)
    dy_buffer = jnp.zeros((N_EP, buffer_rows, D), jnp.bfloat16).at[flat_ids, rows].set(grad_out)
    outs_list, ins_list, gates_list, ups_list, downs_list = [], [], [], [], []
    for expert in range(N_EP):
        x_rows = x_buffer[expert]
        dy_rows = dy_buffer[expert]
        gate_pre = jnp.dot(x_rows, w_gate[expert], preferred_element_type=jnp.float32)
        up_pre = jnp.dot(x_rows, w_up[expert], preferred_element_type=jnp.float32)
        active, slope = silu_parts(gate_pre)
        hidden = (active * up_pre).astype(jnp.bfloat16)
        outs_list.append(rounded_blocks([(hidden, w_down[expert])], buffer_rows))
        grad_hidden = jnp.dot(dy_rows, w_down[expert].T, preferred_element_type=jnp.float32)
        grad_gate_pre = (grad_hidden * up_pre * slope).astype(jnp.bfloat16)
        grad_up_pre = (grad_hidden * active).astype(jnp.bfloat16)
        ins_list.append(rounded_blocks([(grad_gate_pre, w_gate[expert].T), (grad_up_pre, w_up[expert].T)], buffer_rows))
        gates_list.append(jnp.dot(x_rows.T, grad_gate_pre, preferred_element_type=jnp.float32).astype(jnp.bfloat16))
        ups_list.append(jnp.dot(x_rows.T, grad_up_pre, preferred_element_type=jnp.float32).astype(jnp.bfloat16))
        downs_list.append(jnp.dot(hidden.T, dy_rows, preferred_element_type=jnp.float32).astype(jnp.bfloat16))
    expert_out = jnp.stack(outs_list)[flat_ids, rows].reshape(TOKENS, TOP, D).astype(jnp.float32)
    grad_in = jnp.stack(ins_list)[flat_ids, rows].reshape(TOKENS, TOP, D).astype(jnp.float32)
    mixed = jnp.sum(combine_weights[:, :, None] * expert_out, axis=1).astype(jnp.bfloat16)
    grad_combine = jnp.sum(cotangent.astype(jnp.float32)[:, None, :] * expert_out, axis=2)
    grad_tokens = jnp.sum(grad_in, axis=1).astype(jnp.bfloat16)
    return (mixed, grad_tokens, grad_combine, jnp.stack(gates_list), jnp.stack(ups_list), jnp.stack(downs_list))
```

```python
import functools

import jax
import jax.numpy as jnp
from jax import lax
from jax.experimental import pallas as pl
from jax.experimental.pallas import tpu as pltpu
from jax.sharding import PartitionSpec as P

SIDE = 4
CAP = 40
HALF = 48
PAIR = 2 * HALF
GROUPS = 8
ROWS = GROUPS * PAIR
SLOTS = GROUPS * CAP
PACK = 2 * SLOTS
WIN = 384
F32 = jnp.float32
BF16 = jnp.bfloat16
VMEM = pl.BlockSpec(memory_space=pltpu.VMEM)


def dot(a, b, ca, cb):
    return lax.dot_general(a, b, (((ca,), (cb,)), ((), ())), preferred_element_type=F32)


def iota(shape, dim):
    return lax.broadcasted_iota(jnp.int32, shape, dim)


class Grid:
    def __init__(self):
        t = lax.axis_index("tp")
        self.tp = t
        self.c = t % 2
        self.x = (t // 2) % SIDE
        self.y = t // (2 * SIDE)
        self.z = lax.axis_index("ep")

    def at(self, dy, dx, other=False):
        y = (self.y + (dy + SIDE)) % SIDE
        x = (self.x + (dx + SIDE)) % SIDE
        c = 1 - self.c if other else self.c
        return (y * SIDE + x) * 2 + c

    def block(self, h, o1, o2, other=False):
        return self.at(o2, o1, other) if h == 0 else self.at(o1, o2, other)

    def up(self, k):
        return (self.z + k) % GROUPS


class Copies:
    def __init__(self, send, recv):
        self.send, self.recv, self.n, self.ids, self.started = send, recv, 0, {}, []

    def make(self, key, src, dst, to):
        if key not in self.ids:
            self.ids[key] = len(self.ids)
        j = self.ids[key]
        return pltpu.make_async_remote_copy(
            src_ref=src,
            dst_ref=dst,
            send_sem=self.send.at[j],
            recv_sem=self.recv.at[j],
            device_id=to,
            device_id_type=pl.DeviceIdType.MESH,
        )

    def start(self, key, src, dst, to):
        c = self.make(key, src, dst, to)
        c.start()
        self.started.append(c)

    def wait(self, key, dst, to):
        self.make(key, dst, dst, to).wait_recv()

    def finish(self):
        for c in self.started:
            c.wait_send()


def greet(partners):
    barrier = pltpu.get_barrier_semaphore()
    for to in partners:
        pl.semaphore_signal(barrier, inc=1, device_id=to, device_id_type=pl.DeviceIdType.MESH)
    pl.semaphore_wait(barrier, len(partners))


def gather(g, cp, half, part, tick):
    sib = {"tp": g.at(0, 0, True)}

    def nbr(h, axis, d):
        return {"tp": g.block(h, d, 0) if axis == 1 else g.block(h, 0, d)}

    def send(key, h, axis, d, ref):
        cp.start(key, ref, ref, nbr(h, axis, d))

    def got(key, h, axis, d, ref):
        cp.wait(key, ref, nbr(h, axis, d))

    def across(h, o1, o2):
        ref = half(g.block(h, o1, o2), h)
        cp.start(("s", h, o1, o2), ref, ref, sib)

    def from_sib(h, o1, o2):
        b = g.block(h, o1, o2, True)
        cp.wait(("s", h, o1, o2), half(b, h), sib)
        tick(b, h)

    dirs = (1, -1)
    for h in (0, 1):
        for d in dirs:
            send(("p1", h, d), h, 1, d, half(g.tp, h))
    for h in (0, 1):
        for d in dirs:
            send(("p2", h, 0, d), h, 2, d, half(g.tp, h))
    for h in (0, 1):
        across(h, 0, 0)
    yield
    for h in (0, 1):
        tick(g.tp, h)
        from_sib(h, 0, 0)
    for d in dirs:
        for h in (0, 1):
            b = g.block(h, -d, 0)
            got(("p1", h, d), h, 1, -d, half(b, h))
            send(("f1", h, d), h, 1, d, part(b, h, d, 0))
            for e in dirs:
                send(("p2", h, -d, e), h, 2, e, half(b, h))
            across(h, -d, 0)
            tick(b, h)
    yield
    for e in dirs:
        for h in (0, 1):
            b = g.block(h, 0, -e)
            got(("p2", h, 0, e), h, 2, -e, half(b, h))
            send(("f2", h, 0, e), h, 2, e, part(b, h, e, 0))
            across(h, 0, -e)
            tick(b, h)
            from_sib(h, -e, 0)
    yield
    for h in (0, 1):
        b = g.block(h, 2, 0)
        for d in dirs:
            got(("f1", h, d), h, 1, -d, part(b, h, d, 0))
        for e in dirs:
            send(("p2", h, 2, e), h, 2, e, half(b, h))
        across(h, 2, 0)
        tick(b, h)
        from_sib(h, 0, -1)
        from_sib(h, 0, 1)
    yield
    for o1 in (-1, 1):
        for e in dirs:
            for h in (0, 1):
                b = g.block(h, o1, -e)
                got(("p2", h, o1, e), h, 2, -e, half(b, h))
                send(("f2", h, o1, e), h, 2, e, part(b, h, e, o1))
                across(h, o1, -e)
                tick(b, h)
                if (o1, e) == (-1, 1):
                    from_sib(h, 2, 0)
    yield
    for h in (0, 1):
        b = g.block(h, 0, 2)
        for e in dirs:
            got(("f2", h, 0, e), h, 2, -e, part(b, h, e, 0))
        across(h, 0, 2)
        tick(b, h)
        for o1 in (-1, 1):
            for e in dirs:
                from_sib(h, o1, -e)
    yield
    for e in dirs:
        for h in (0, 1):
            b = g.block(h, 2, -e)
            got(("p2", h, 2, e), h, 2, -e, half(b, h))
            send(("f2", h, 2, e), h, 2, e, part(b, h, e, 2))
            across(h, 2, -e)
            tick(b, h)
            if e == 1:
                from_sib(h, 0, 2)
    yield
    for o1 in (-1, 1):
        for h in (0, 1):
            b = g.block(h, o1, 2)
            for e in dirs:
                got(("f2", h, o1, e), h, 2, -e, part(b, h, e, o1))
            across(h, o1, 2)
            tick(b, h)
            from_sib(h, 2, -o1)
    yield
    for h in (0, 1):
        b = g.block(h, 2, 2)
        for e in dirs:
            got(("f2", h, 2, e), h, 2, -e, part(b, h, e, 2))
        across(h, 2, 2)
        tick(b, h)
        from_sib(h, -1, 2)
        from_sib(h, 1, 2)
    for h in (0, 1):
        from_sib(h, 2, 2)
    yield


def places(ids):
    n = ids.shape[0]
    lane = iota((n, 128), 1)
    before = (iota((n, n), 1) < iota((n, n), 0)).astype(BF16)
    hot = [(ids[:, k : k + 1] == lane).astype(F32) for k in (0, 1)]
    seen = [dot(before, hot[k].astype(BF16), 1, 0) for k in (0, 1)]
    seen[1] = seen[1] + jnp.sum(hot[0], axis=0, keepdims=True)
    rank = [jnp.sum(seen[k] * hot[k], axis=1, keepdims=True) for k in (0, 1)]
    row = [ids[:, k : k + 1].astype(F32) * PAIR + rank[k] for k in (0, 1)]
    lanes = iota((n, ROWS), 1).astype(F32)
    first = [(lanes == row[k]).astype(BF16) for k in (0, 1)]
    second = [(lanes == row[k] + HALF).astype(BF16) for k in (0, 1)]
    return first, second


def packing():
    r = iota((ROWS, PACK), 0)
    lane = iota((ROWS, PACK), 1)
    j = r % PAIR
    grad = j >= HALF
    k = jnp.where(grad, j - HALF, j)
    s = (r // PAIR) * CAP + k
    want = jnp.where(grad, jnp.where(s < 256, s + 384, s + 64), s)
    return ((want == lane) & (k < CAP)).astype(BF16)


def to_all_groups(g, cp, src, dst, name):
    for k in range(1, GROUPS):
        to = g.up(k)
        cp.start(
            (name, k),
            src.at[pl.ds(pl.multiple_of(to * PAIR, PAIR), PAIR)],
            dst.at[pl.ds(pl.multiple_of(g.z * PAIR, PAIR), PAIR)],
            {"ep": to},
        )


def from_all_groups(g, cp, dst, name):
    for k in range(1, GROUPS):
        frm = g.up(GROUPS - k)
        cp.wait((name, k), dst.at[pl.ds(pl.multiple_of(frm * PAIR, PAIR), PAIR)], {"ep": frm})


def own_group(g, src, dst):
    mine = pl.ds(pl.multiple_of(g.z * PAIR, PAIR), PAIR)
    dst[mine] = src[mine]


def dispatch_kernel(tok_ref, cot_ref, ids_ref, w_ref, own_ref, all_ref, rows, got, send, recv):
    g = Grid()
    cp = Copies(send, recv)
    greet(
        [{"tp": g.at(0, 0, True)}]
        + [{"tp": g.at(*o)} for o in ((0, 1), (0, -1), (1, 0), (-1, 0))]
        + [{"ep": g.up(k)} for k in range(1, GROUPS)]
    )
    first, second = places(ids_ref[...])
    cot = cot_ref[...].astype(F32)
    w = w_ref[...]
    scaled = [(w[:, k : k + 1] * cot).astype(BF16) for k in (0, 1)]
    sent = dot(first[0] + first[1], tok_ref[...], 0, 0)
    sent = sent + dot(second[0], scaled[0], 0, 0) + dot(second[1], scaled[1], 0, 0)
    rows[...] = sent.astype(BF16)
    to_all_groups(g, cp, rows, got, "out")
    own_group(g, rows, got)
    pack = packing()
    from_all_groups(g, cp, got, "out")
    own = dot(got[...], pack, 0, 0).astype(BF16)
    own_ref[...] = own
    size = own.shape[0]
    all_ref[pl.ds(pl.multiple_of(g.tp * size, size), size), :] = own
    hh = size // 2

    def half(b, h):
        return all_ref.at[pl.ds(pl.multiple_of(b * size + h * hh, 16), hh)]

    def part(b, h, q, o):
        low = (q > 0) == (o in (0, 1))
        rng = pl.ds(0, 384) if low else pl.ds(384, 256)
        return all_ref.at[pl.ds(pl.multiple_of(b * size + h * hh, 16), hh), rng]

    for _ in gather(g, cp, half, part, lambda b, h: None):
        pass
    cp.finish()


N_DISPATCH = 7 + 40 + 32


def dispatch(tokens, cotangent, ids, weights):
    width = tokens.shape[1]
    return pl.pallas_call(
        dispatch_kernel,
        out_shape=(
            jax.ShapeDtypeStruct((width, PACK), BF16),
            jax.ShapeDtypeStruct((2 * SIDE * SIDE * width, PACK), BF16),
        ),
        in_specs=[VMEM] * 4,
        out_specs=(VMEM, VMEM),
        scratch_shapes=[
            pltpu.VMEM((ROWS, width), BF16),
            pltpu.VMEM((ROWS, width), BF16),
            pltpu.SemaphoreType.DMA((N_DISPATCH,)),
            pltpu.SemaphoreType.DMA((N_DISPATCH,)),
        ],
        compiler_params=pltpu.CompilerParams(
            collective_id=0, has_side_effects=True, vmem_limit_bytes=60 * 2**20
        ),
        name="dispatch",
    )(tokens, cotangent, ids, weights)


def back_kernel(
    part_ref, act_ref, xg_ref, xu_ref, dy_ref, cot_ref, ids_ref, w_ref,
    gate_ref, up_ref, down_ref, mixed_ref, gt_ref, gc_ref,
    full, sib, chip, ra, rb, mid, fin, rows, got, red, send, recv,
):
    g = Grid()
    cp = Copies(send, recv)
    ring = ((0, 1), (0, -1), (0, 2), (1, 0), (-1, 0), (2, 0))
    greet(
        [{"tp": g.at(0, 0, True)}]
        + [{"tp": g.at(*o)} for o in ring]
        + [{"ep": g.up(k)} for k in range(1, GROUPS)]
    )
    size = act_ref.shape[0]
    hh = size // 2
    width = part_ref.shape[2]
    half_w = width // 2
    sib_dev = {"tp": g.at(0, 0, True)}

    def half(b, h):
        return full.at[pl.ds(pl.multiple_of(b * size + h * hh, 64), hh)]

    def part(b, h, q, o):
        off = 0 if q > 0 else hh // 2
        return full.at[pl.ds(pl.multiple_of(b * size + h * hh + off, 64), hh // 2)]

    def tick(b, h):
        at = pl.multiple_of(b * size + h * hh, 128)
        blk = full[pl.ds(at, hh), :]
        down_ref[pl.ds(at, hh), :] = dot(blk[:, :WIN], dy_ref[...], 1, 0).astype(BF16)
        gate_ref[:, pl.ds(at, hh)] = dot(xg_ref[...], blk[:, 256:640], 1, 1).astype(BF16)
        up_ref[:, pl.ds(at, hh)] = dot(xu_ref[...], blk[:, 640:], 1, 1).astype(BF16)

    cp.start("pair", part_ref.at[:, 1 - g.c], sib, sib_dev)
    mine = pl.ds(pl.multiple_of(g.tp * size, 256), size)
    full[mine, :] = act_ref[...]
    cp.wait("pair", sib, sib_dev)

    def add_pair(i, _):
        chip[i] = (part_ref[i, g.c].astype(F32) + sib[i].astype(F32)).astype(BF16)
        return _

    lax.fori_loop(0, SIDE * SIDE, add_pair, 0)

    def y_of(d):
        return (g.y + d + SIDE) % SIDE

    def x_of(d):
        return (g.x + d + SIDE) % SIDE

    lo, hi = pl.ds(0, half_w), pl.ds(half_w, half_w)
    for i, d in enumerate((1, -1, 2)):
        cp.start(("a1", d), chip.at[pl.ds(y_of(d) * SIDE, SIDE), lo], ra.at[i], {"tp": g.at(d, 0)})
        for r in range(SIDE):
            cp.start(("b1", d, r), chip.at[r * SIDE + x_of(d), hi], rb.at[i, r], {"tp": g.at(0, d)})
    steps = gather(g, cp, half, part, tick)
    next(steps)
    for i, d in enumerate((1, -1, 2)):
        cp.wait(("a1", d), ra.at[i], {"tp": g.at(-d, 0)})
        for r in range(SIDE):
            cp.wait(("b1", d, r), rb.at[i, r], {"tp": g.at(0, -d)})

    def add_a(r, _):
        s = chip[g.y * SIDE + r, lo, :].astype(F32)
        for i in range(3):
            s = s + ra[i, r].astype(F32)
        mid[0, r] = s.astype(BF16)
        s = chip[r * SIDE + g.x, hi, :].astype(F32)
        for i in range(3):
            s = s + rb[i, r].astype(F32)
        mid[1, r] = s.astype(BF16)
        return _

    lax.fori_loop(0, SIDE, add_a, 0)
    for i, d in enumerate((1, -1, 2)):
        cp.start(("a2", d), mid.at[0, x_of(d)], fin.at[0, i], {"tp": g.at(0, d)})
        cp.start(("b2", d), mid.at[1, y_of(d)], fin.at[1, i], {"tp": g.at(d, 0)})
    next(steps)
    next(steps)
    for i, d in enumerate((1, -1, 2)):
        cp.wait(("a2", d), fin.at[0, i], {"tp": g.at(0, -d)})
        cp.wait(("b2", d), fin.at[1, i], {"tp": g.at(-d, 0)})
    sums = []
    for h in (0, 1):
        s = mid[h, g.x if h == 0 else g.y].astype(F32)
        for i in range(3):
            s = s + fin[h, i].astype(F32)
        sums.append(s)
    own = jnp.concatenate(sums, axis=0).astype(BF16)
    rows[...] = dot(packing(), own, 1, 1).astype(BF16)
    to_all_groups(g, cp, rows, got, "back")
    own_group(g, rows, got)
    next(steps)
    first, second = places(ids_ref[...])
    from_all_groups(g, cp, got, "back")
    back = got[...]
    cot = cot_ref[...].astype(F32)
    w = w_ref[...]
    outs = [dot(first[k], back, 1, 0) for k in (0, 1)]
    mixed_ref[...] = (w[:, 0:1] * outs[0] + w[:, 1:2] * outs[1]).astype(BF16)
    gt_ref[...] = (dot(second[0], back, 1, 0) + dot(second[1], back, 1, 0)).astype(BF16)
    inner = [jnp.sum(cot * outs[k], axis=1, keepdims=True) for k in (0, 1)]
    lane = iota((inner[0].shape[0], 128), 1)
    red[0] = jnp.where(lane == 0, inner[0], jnp.where(lane == 1, inner[1], 0.0))
    cp.start("g0", red.at[0], red.at[1], sib_dev)
    next(steps)
    cp.wait("g0", red.at[1], sib_dev)
    red[2 + g.x] = red[0] + red[1]
    for d in (1, -1, 2):
        cp.start(("g1", d), red.at[2 + g.x], red.at[2 + g.x], {"tp": g.at(0, d)})
    next(steps)
    for d in (1, -1, 2):
        cp.wait(("g1", d), red.at[2 + x_of(-d)], {"tp": g.at(0, -d)})
    red[6 + g.y] = (red[2] + red[3]) + (red[4] + red[5])
    for d in (1, -1, 2):
        cp.start(("g2", d), red.at[6 + g.y], red.at[6 + g.y], {"tp": g.at(d, 0)})
    for _ in steps:
        pass
    for d in (1, -1, 2):
        cp.wait(("g2", d), red.at[6 + y_of(-d)], {"tp": g.at(-d, 0)})
    gc_ref[...] = ((red[6] + red[7]) + (red[8] + red[9]))[:, :2]
    cp.finish()


N_BACK = 1 + 15 + 72 + 6 + 7 + 7


def back(part, act, xg, xu, dy, cotangent, ids, weights):
    width = cotangent.shape[1]
    size = act.shape[0]
    n = 2 * SIDE * SIDE
    return pl.pallas_call(
        back_kernel,
        out_shape=(
            jax.ShapeDtypeStruct((width, n * size), BF16),
            jax.ShapeDtypeStruct((width, n * size), BF16),
            jax.ShapeDtypeStruct((n * size, width), BF16),
            jax.ShapeDtypeStruct(cotangent.shape, BF16),
            jax.ShapeDtypeStruct(cotangent.shape, BF16),
            jax.ShapeDtypeStruct(ids.shape, F32),
        ),
        in_specs=[VMEM] * 8,
        out_specs=(VMEM,) * 6,
        scratch_shapes=[
            pltpu.VMEM((n * size, act.shape[1]), BF16),
            pltpu.VMEM((SIDE * SIDE, width, PACK), BF16),
            pltpu.VMEM((SIDE * SIDE, width, PACK), BF16),
            pltpu.VMEM((3, SIDE, width // 2, PACK), BF16),
            pltpu.VMEM((3, SIDE, width // 2, PACK), BF16),
            pltpu.VMEM((2, SIDE, width // 2, PACK), BF16),
            pltpu.VMEM((2, 3, width // 2, PACK), BF16),
            pltpu.VMEM((ROWS, width), BF16),
            pltpu.VMEM((ROWS, width), BF16),
            pltpu.VMEM((10, width, 128), F32),
            pltpu.SemaphoreType.DMA((N_BACK,)),
            pltpu.SemaphoreType.DMA((N_BACK,)),
        ],
        compiler_params=pltpu.CompilerParams(
            collective_id=1, has_side_effects=True, vmem_limit_bytes=60 * 2**20
        ),
        name="back",
    )(part, act, xg, xu, dy, cotangent, ids, weights)


def body(tokens, cotangent, expert_ids, combine_weights, w_gate, w_up, w_down):
    width = tokens.shape[1]
    gate_w, up_w, down_w = w_gate[0], w_up[0], w_down[0]
    own, xd = dispatch(tokens, cotangent, expert_ids, combine_weights)
    gate_pre = dot(gate_w, xd[:, :WIN], 0, 0)
    up_pre = dot(up_w, xd[:, :WIN], 0, 0)
    gh = dot(down_w, xd[:, 256:], 1, 0)
    gh = jnp.concatenate([gh[:, 128:], gh[:, 64:128], gh[:, 0:64]], axis=1)
    live = iota(gh.shape, 1) < SLOTS
    sigma = jax.nn.sigmoid(gate_pre)
    active = gate_pre * sigma
    slope = sigma * (1.0 + gate_pre * (1.0 - sigma))
    hidden = jnp.where(live, active * up_pre, 0.0).astype(BF16)
    ggp = jnp.where(live, gh * up_pre * slope, 0.0).astype(BF16)
    gup = jnp.where(live, gh * active, 0.0).astype(BF16)
    act = jnp.concatenate([hidden[:, :SLOTS], ggp[:, 256:SLOTS], ggp[:, :256], gup], axis=1)
    out = dot(down_w, hidden[:, :SLOTS], 0, 0).astype(BF16)
    grad = (dot(gate_w, ggp[:, :SLOTS], 1, 0) + dot(up_w, gup[:, :SLOTS], 1, 0)).astype(BF16)
    part = jnp.concatenate([out, grad[:, 256:], grad[:, :256]], axis=1)
    part = part.reshape(SIDE * SIDE, 2, width, PACK)
    zero = jnp.zeros((width, 64), BF16)
    xg = jnp.concatenate([zero, own[:, 256:320], own[:, :256]], axis=1)
    xu = jnp.concatenate([own[:, :320], zero], axis=1)
    dy = jnp.concatenate([own[:, 384:], own[:, 320:384], zero], axis=1).T
    gate, up, down, mixed, gt, gc = back(
        part, act, xg, xu, dy, cotangent, expert_ids, combine_weights
    )
    return mixed, gt, gc, gate[None], up[None], down[None]


def solution(mesh):
    placed = (
        P("ep", "tp"),
        P("ep", "tp"),
        P("ep", None),
        P("ep", None),
        P("ep", None, "tp"),
        P("ep", None, "tp"),
        P("ep", "tp", None),
    )
    return jax.shard_map(
        body,
        mesh=mesh,
        in_specs=placed,
        out_specs=(
            P("ep", "tp"),
            P("ep", "tp"),
            P("ep", None),
            P("ep", "tp", None),
            P("ep", "tp", None),
            P("ep", None, "tp"),
        ),
        check_vma=False,
    )
```

```python
import functools

import jax
import jax.numpy as jnp
from jax import lax
from jax.experimental import pallas as pl
from jax.experimental.pallas import tpu as pltpu
from jax.sharding import PartitionSpec as P

SIDE = 4
CAP = 40
HALF = CAP
PAIR = 2 * HALF
GROUPS = 8
ROWS = GROUPS * PAIR
SLOTS = GROUPS * CAP
PACK = 2 * SLOTS
WIN = 384
F32 = jnp.float32
BF16 = jnp.bfloat16
VMEM = pl.BlockSpec(memory_space=pltpu.VMEM)


def dot(a, b, ca, cb):
    return lax.dot_general(a, b, (((ca,), (cb,)), ((), ())), preferred_element_type=F32)


def iota(shape, dim):
    return lax.broadcasted_iota(jnp.int32, shape, dim)


class Grid:
    def __init__(self):
        t = lax.axis_index("tp")
        self.tp = t
        self.c = t % 2
        self.x = (t // 2) % SIDE
        self.y = t // (2 * SIDE)
        self.z = lax.axis_index("ep")

    def at(self, dy, dx, other=False):
        y = (self.y + (dy + SIDE)) % SIDE
        x = (self.x + (dx + SIDE)) % SIDE
        c = 1 - self.c if other else self.c
        return (y * SIDE + x) * 2 + c

    def block(self, h, o1, o2, other=False):
        return self.at(o2, o1, other) if h == 0 else self.at(o1, o2, other)

    def up(self, k):
        return (self.z + k) % GROUPS


class Copies:
    def __init__(self, send, recv):
        self.send, self.recv, self.n, self.ids, self.started = send, recv, 0, {}, []

    def make(self, key, src, dst, to):
        if key not in self.ids:
            self.ids[key] = len(self.ids)
        j = self.ids[key]
        return pltpu.make_async_remote_copy(
            src_ref=src,
            dst_ref=dst,
            send_sem=self.send.at[j],
            recv_sem=self.recv.at[j],
            device_id=to,
            device_id_type=pl.DeviceIdType.MESH,
        )

    def start(self, key, src, dst, to):
        c = self.make(key, src, dst, to)
        c.start()
        self.started.append(c)

    def wait(self, key, dst, to):
        self.make(key, dst, dst, to).wait_recv()

    def finish(self):
        for c in self.started:
            c.wait_send()


def greet(partners):
    barrier = pltpu.get_barrier_semaphore()
    for to in partners:
        pl.semaphore_signal(barrier, inc=1, device_id=to, device_id_type=pl.DeviceIdType.MESH)


def greeted(partners):
    pl.semaphore_wait(pltpu.get_barrier_semaphore(), len(partners))


def gather(g, cp, name, half, part, tick):
    sib = {"tp": g.at(0, 0, True)}

    def nbr(h, axis, d):
        return {"tp": g.block(h, d, 0) if axis == 1 else g.block(h, 0, d)}

    def send(key, h, axis, d, ref):
        cp.start((name, *key), ref, ref, nbr(h, axis, d))

    def got(key, h, axis, d, ref):
        cp.wait((name, *key), ref, nbr(h, axis, d))

    def across(h, o1, o2):
        ref = half(g.block(h, o1, o2), h)
        cp.start((name, "s", h, o1, o2), ref, ref, sib)

    def from_sib(h, o1, o2):
        b = g.block(h, o1, o2, True)
        cp.wait((name, "s", h, o1, o2), half(b, h), sib)
        tick(b, h)

    dirs = (1, -1)
    for h in (0, 1):
        for d in dirs:
            send(("p1", h, d), h, 1, d, half(g.tp, h))
    for h in (0, 1):
        for d in dirs:
            send(("p2", h, 0, d), h, 2, d, half(g.tp, h))
    for h in (0, 1):
        across(h, 0, 0)
    yield
    for h in (0, 1):
        tick(g.tp, h)
        from_sib(h, 0, 0)
    for d in dirs:
        for h in (0, 1):
            b = g.block(h, -d, 0)
            got(("p1", h, d), h, 1, -d, half(b, h))
            send(("f1", h, d), h, 1, d, part(b, h, d, 0))
            for e in dirs:
                send(("p2", h, -d, e), h, 2, e, half(b, h))
            across(h, -d, 0)
            tick(b, h)
    yield
    for e in dirs:
        for h in (0, 1):
            b = g.block(h, 0, -e)
            got(("p2", h, 0, e), h, 2, -e, half(b, h))
            send(("f2", h, 0, e), h, 2, e, part(b, h, e, 0))
            across(h, 0, -e)
            tick(b, h)
            from_sib(h, -e, 0)
    yield
    for h in (0, 1):
        b = g.block(h, 2, 0)
        for d in dirs:
            got(("f1", h, d), h, 1, -d, part(b, h, d, 0))
        for e in dirs:
            send(("p2", h, 2, e), h, 2, e, half(b, h))
        across(h, 2, 0)
        tick(b, h)
        from_sib(h, 0, -1)
        from_sib(h, 0, 1)
    yield
    for o1 in (-1, 1):
        for e in dirs:
            for h in (0, 1):
                b = g.block(h, o1, -e)
                got(("p2", h, o1, e), h, 2, -e, half(b, h))
                send(("f2", h, o1, e), h, 2, e, part(b, h, e, o1))
                across(h, o1, -e)
                tick(b, h)
                if (o1, e) == (-1, 1):
                    from_sib(h, 2, 0)
    yield
    for h in (0, 1):
        b = g.block(h, 0, 2)
        for e in dirs:
            got(("f2", h, 0, e), h, 2, -e, part(b, h, e, 0))
        across(h, 0, 2)
        tick(b, h)
        for o1 in (-1, 1):
            for e in dirs:
                from_sib(h, o1, -e)
    yield
    for e in dirs:
        for h in (0, 1):
            b = g.block(h, 2, -e)
            got(("p2", h, 2, e), h, 2, -e, half(b, h))
            send(("f2", h, 2, e), h, 2, e, part(b, h, e, 2))
            across(h, 2, -e)
            tick(b, h)
            if e == 1:
                from_sib(h, 0, 2)
    yield
    for o1 in (-1, 1):
        for h in (0, 1):
            b = g.block(h, o1, 2)
            for e in dirs:
                got(("f2", h, o1, e), h, 2, -e, part(b, h, e, o1))
            across(h, o1, 2)
            tick(b, h)
            from_sib(h, 2, -o1)
    yield
    for h in (0, 1):
        b = g.block(h, 2, 2)
        for e in dirs:
            got(("f2", h, 2, e), h, 2, -e, part(b, h, e, 2))
        across(h, 2, 2)
        tick(b, h)
        from_sib(h, -1, 2)
        from_sib(h, 1, 2)
    for h in (0, 1):
        from_sib(h, 2, 2)
    yield


def column(row):
    n = row.shape[1]
    eye = iota((n, n), 0) == iota((n, n), 1)
    return jnp.sum(jnp.where(eye, row, jnp.zeros_like(row)), axis=1, keepdims=True)


def as_row(col):
    n = col.shape[0]
    eye = iota((n, n), 0) == iota((n, n), 1)
    return jnp.sum(jnp.where(eye, col, jnp.zeros_like(col)), axis=0, keepdims=True)


def places(ids):
    n = ids[0].shape[0]
    lane = iota((n, 128), 1).astype(F32)
    before = (iota((n, n), 1) < iota((n, n), 0)).astype(BF16)
    hot = [(ids[k] == lane).astype(F32) for k in (0, 1)]
    seen = [dot(before, hot[k].astype(BF16), 1, 0) for k in (0, 1)]
    seen[1] = seen[1] + jnp.sum(hot[0], axis=0, keepdims=True)
    rank = [jnp.sum(seen[k] * hot[k], axis=1, keepdims=True) for k in (0, 1)]
    row = [ids[k] * PAIR + rank[k] for k in (0, 1)]
    lanes = iota((n, ROWS), 1).astype(F32)
    first = [(lanes == row[k]).astype(BF16) for k in (0, 1)]
    second = [(lanes == row[k] + HALF).astype(BF16) for k in (0, 1)]
    return first, second


def fill_packing(pack):
    j = iota((PAIR, 1), 0)
    lane = iota((PAIR, PACK), 1)
    for z in range(GROUPS):
        s = z * CAP + j
        d = s - CAP
        want = jnp.where(j >= CAP, jnp.where(d < 256, d + 384, d + 64), s)
        pack[z * PAIR : (z + 1) * PAIR, :] = (want == lane).astype(F32).astype(BF16)


def to_all_groups(g, cp, src, dst, name):
    for k in range(1, GROUPS):
        to = g.up(k)
        cp.start(
            (name, k),
            src.at[pl.ds(pl.multiple_of(to * PAIR, PAIR), PAIR)],
            dst.at[pl.ds(pl.multiple_of(g.z * PAIR, PAIR), PAIR)],
            {"ep": to},
        )


def from_all_groups(g, cp, dst, name):
    for k in range(1, GROUPS):
        frm = g.up(GROUPS - k)
        cp.wait((name, k), dst.at[pl.ds(pl.multiple_of(frm * PAIR, PAIR), PAIR)], {"ep": frm})


def own_group(g, src, dst):
    mine = pl.ds(pl.multiple_of(g.z * PAIR, PAIR), PAIR)
    dst[mine] = src[mine]


def turned(t):
    return pltpu.roll(t, 64, 1)


def layer_kernel(
    tok_ref, cot_ref, ids_ref, w_ref, gw_hbm, uw_hbm, dw_hbm,
    gate_ref, up_ref, down_ref, mixed_ref, gt_ref, gc_ref,
    gw, uw, dw, gwt, uwt, dwt, pack, all_ref, win, hx, gy, uy,
    full, part_ref, sib, chip, ra, rb, mid, fin, rows, got, rows2, got2, red, local, send, recv,
):
    g = Grid()
    cp = Copies(send, recv)
    sib_dev = {"tp": g.at(0, 0, True)}
    ring = ((0, 1), (0, -1), (0, 2), (1, 0), (-1, 0), (2, 0))
    partners = (
        [sib_dev] + [{"tp": g.at(*o)} for o in ring] + [{"ep": g.up(k)} for k in range(1, GROUPS)]
    )
    greet(partners)
    loads = [
        pltpu.make_async_copy(a, b, local.at[i])
        for i, (a, b) in enumerate(((gw_hbm, gw), (uw_hbm, uw), (dw_hbm, dw)))
    ]
    for c in loads:
        c.start()

    width = tok_ref.shape[1]
    ids = [column(ids_ref[k : k + 1, :].astype(F32)) for k in (0, 1)]
    w = [column(w_ref[k : k + 1, :]) for k in (0, 1)]
    first, second = places(ids)
    cot = cot_ref[...].astype(F32)
    scaled = [(w[k] * cot).astype(BF16) for k in (0, 1)]
    sent = dot(first[0] + first[1], tok_ref[...], 0, 0)
    sent = sent + dot(second[0], scaled[0], 0, 0) + dot(second[1], scaled[1], 0, 0)
    rows[...] = sent.astype(BF16)
    greeted(partners)
    to_all_groups(g, cp, rows, got, "out")
    own_group(g, rows, got)
    fill_packing(pack)
    for c in loads:
        c.wait()
    size = gw.shape[1]
    blocks = gw.shape[0] // width

    def turn(i, _):
        at = pl.ds(pl.multiple_of(i * 256, 256), 256)
        gwt[:, at] = gw[at, :].T
        uwt[:, at] = uw[at, :].T
        dwt[at, :] = dw[:, at].T
        return _

    lax.fori_loop(0, gw.shape[0] // 256, turn, 0)
    from_all_groups(g, cp, got, "out")
    own = dot(got[...], pack[...], 0, 0)
    all_ref[pl.ds(pl.multiple_of(g.tp * width, width), width), :] = own.astype(BF16)
    low = iota((width, 128), 1) < 64
    o = [own[:, i * 128 : (i + 1) * 128] for i in range(5)]
    x2 = jnp.where(low, o[2], 0.0)
    d2 = jnp.where(low, turned(o[2]), 0.0)
    for i, t in enumerate((turned(x2), o[0], o[1])):
        win[0, :, i * 128 : (i + 1) * 128] = t.astype(BF16)
    for i, t in enumerate((o[0], o[1], x2)):
        win[1, :, i * 128 : (i + 1) * 128] = t.astype(BF16)
    for i, t in enumerate((o[3], o[4], d2)):
        win[2, :, i * 128 : (i + 1) * 128] = t.astype(BF16)
    half_w = width // 2

    def half_in(b, h):
        return all_ref.at[pl.ds(pl.multiple_of(b * width + h * half_w, 16), half_w)]

    def part_in(b, h, q, o):
        rng = pl.ds(0, 384) if (q > 0) == (o in (0, 1)) else pl.ds(384, 256)
        return all_ref.at[pl.ds(pl.multiple_of(b * width + h * half_w, 16), half_w), rng]

    for _ in gather(g, cp, "in", half_in, part_in, lambda b, h: None):
        pass

    hh = size // 2
    mine = g.tp * size

    def units(h, _):
        r = pl.ds(pl.multiple_of(h * hh, hh), hh)
        gate = dot(gwt[r, :], all_ref[:, :WIN], 1, 0)
        upp = dot(uwt[r, :], all_ref[:, :WIN], 1, 0)
        gh = dot(dw[r, :], all_ref[:, 256:], 1, 0)
        at = pl.ds(pl.multiple_of(mine + h * hh, hh), hh)
        lo = iota((hh, 128), 1) < 64
        for i in range(3):
            t = slice(i * 128, (i + 1) * 128)
            gp, u = gate[:, t], upp[:, t]
            d = turned(gh[:, 0:128]) if i == 2 else gh[:, (i + 1) * 128 : (i + 2) * 128]
            s = jax.nn.sigmoid(gp)
            active = gp * s
            hid = active * u
            gg = d * u * (s * (1.0 + gp * (1.0 - s)))
            gu = d * active
            if i == 2:
                hid, gg, gu = (jnp.where(lo, a, 0.0) for a in (hid, gg, gu))
                full[at, 256:384] = (hid + turned(gg)).astype(BF16)
                gy[r, 0:128] = turned(gg).astype(BF16)
                uy[r, 0:128] = turned(gu).astype(BF16)
            else:
                full[at, t] = hid.astype(BF16)
                full[at, 384 + i * 128 : 512 + i * 128] = gg.astype(BF16)
                gy[r, (i + 1) * 128 : (i + 2) * 128] = gg.astype(BF16)
                uy[r, (i + 1) * 128 : (i + 2) * 128] = gu.astype(BF16)
            hx[r, t] = hid.astype(BF16)
            full[at, 640 + i * 128 : 768 + i * 128] = gu.astype(BF16)
        return _

    lax.fori_loop(0, 2, units, 0)

    def half(b, h):
        return full.at[pl.ds(pl.multiple_of(b * size + h * hh, 64), hh)]

    def part(b, h, q, o):
        off = 0 if q > 0 else hh // 2
        return full.at[pl.ds(pl.multiple_of(b * size + h * hh + off, 64), hh // 2)]

    def tick(b, h):
        at = pl.multiple_of(b * size + h * hh, 128)
        blk = full[pl.ds(at, hh), :]
        gate_ref[:, pl.ds(at, hh)] = dot(win[0], blk[:, 256:640], 1, 1).astype(BF16)
        up_ref[:, pl.ds(at, hh)] = dot(win[1], blk[:, 640:], 1, 1).astype(BF16)
        down_ref[:, pl.ds(at, hh)] = dot(win[2], blk[:, :WIN], 1, 1).astype(BF16)

    steps = gather(g, cp, "act", half, part, tick)
    next(steps)

    def partial(c):
        def one(i, _):
            at = pl.ds(pl.multiple_of((2 * i + c) * width, width), width)
            out = dot(dwt[at, :], hx[...], 1, 0)
            inn = dot(gw[at, :], gy[...], 1, 0) + dot(uw[at, :], uy[...], 1, 0)
            part_ref[c, i, :, 0:256] = out[:, 0:256].astype(BF16)
            part_ref[c, i, :, 256:384] = (out[:, 256:] + inn[:, :128]).astype(BF16)
            part_ref[c, i, :, 384:640] = inn[:, 128:].astype(BF16)
            return _

        lax.fori_loop(0, blocks // 2, one, 0)

    partial(1 - g.c)
    cp.start("pair", part_ref.at[1 - g.c], sib, sib_dev)
    partial(g.c)
    cp.wait("pair", sib, sib_dev)

    def add_pair(i, _):
        chip[i] = (part_ref[g.c, i].astype(F32) + sib[i].astype(F32)).astype(BF16)
        return _

    lax.fori_loop(0, SIDE * SIDE, add_pair, 0)

    def y_of(d):
        return (g.y + d + SIDE) % SIDE

    def x_of(d):
        return (g.x + d + SIDE) % SIDE

    lo, hi = pl.ds(0, half_w), pl.ds(half_w, half_w)
    for i, d in enumerate((1, -1, 2)):
        cp.start(("a1", d), chip.at[pl.ds(y_of(d) * SIDE, SIDE), lo], ra.at[i], {"tp": g.at(d, 0)})
        for r in range(SIDE):
            cp.start(("b1", d, r), chip.at[r * SIDE + x_of(d), hi], rb.at[i, r], {"tp": g.at(0, d)})
    next(steps)
    for i, d in enumerate((1, -1, 2)):
        cp.wait(("a1", d), ra.at[i], {"tp": g.at(-d, 0)})
        for r in range(SIDE):
            cp.wait(("b1", d, r), rb.at[i, r], {"tp": g.at(0, -d)})

    def add_a(r, _):
        s = chip[g.y * SIDE + r, lo, :].astype(F32)
        for i in range(3):
            s = s + ra[i, r].astype(F32)
        mid[0, r] = s.astype(BF16)
        s = chip[r * SIDE + g.x, hi, :].astype(F32)
        for i in range(3):
            s = s + rb[i, r].astype(F32)
        mid[1, r] = s.astype(BF16)
        return _

    lax.fori_loop(0, SIDE, add_a, 0)
    for i, d in enumerate((1, -1, 2)):
        cp.start(("a2", d), mid.at[0, x_of(d)], fin.at[0, i], {"tp": g.at(0, d)})
        cp.start(("b2", d), mid.at[1, y_of(d)], fin.at[1, i], {"tp": g.at(d, 0)})
    next(steps)
    next(steps)
    for i, d in enumerate((1, -1, 2)):
        cp.wait(("a2", d), fin.at[0, i], {"tp": g.at(0, -d)})
        cp.wait(("b2", d), fin.at[1, i], {"tp": g.at(-d, 0)})
    sums = []
    for h in (0, 1):
        s = mid[h, g.x if h == 0 else g.y].astype(F32)
        for i in range(3):
            s = s + fin[h, i].astype(F32)
        sums.append(s)
    total = jnp.concatenate(sums, axis=0).astype(BF16)
    rows2[...] = dot(pack[...], total, 1, 1).astype(BF16)
    to_all_groups(g, cp, rows2, got2, "back")
    own_group(g, rows2, got2)
    next(steps)
    from_all_groups(g, cp, got2, "back")
    back = got2[...]
    outs = [dot(first[k], back, 1, 0) for k in (0, 1)]
    mixed_ref[...] = (w[0] * outs[0] + w[1] * outs[1]).astype(BF16)
    gt_ref[...] = (dot(second[0], back, 1, 0) + dot(second[1], back, 1, 0)).astype(BF16)
    inner = [as_row(jnp.sum(cot * outs[k], axis=1, keepdims=True)) for k in (0, 1)]
    sub = iota((8, width), 0)
    red[0] = jnp.zeros((8, 128), F32)
    red[0, :, 0:width] = jnp.where(sub == 0, inner[0], jnp.where(sub == 1, inner[1], 0.0))
    cp.start("g0", red.at[0], red.at[1], sib_dev)
    next(steps)
    cp.wait("g0", red.at[1], sib_dev)
    red[2 + g.x] = red[0] + red[1]
    for d in (1, -1, 2):
        cp.start(("g1", d), red.at[2 + g.x], red.at[2 + g.x], {"tp": g.at(0, d)})
    next(steps)
    for d in (1, -1, 2):
        cp.wait(("g1", d), red.at[2 + x_of(-d)], {"tp": g.at(0, -d)})
    red[6 + g.y] = (red[2] + red[3]) + (red[4] + red[5])
    for d in (1, -1, 2):
        cp.start(("g2", d), red.at[6 + g.y], red.at[6 + g.y], {"tp": g.at(d, 0)})
    for _ in steps:
        pass
    for d in (1, -1, 2):
        cp.wait(("g2", d), red.at[6 + y_of(-d)], {"tp": g.at(-d, 0)})
    gc_ref[...] = ((red[6] + red[7]) + (red[8] + red[9]))[0:2, 0:width]
    cp.finish()


N_COPIES = 2 * 7 + 2 * (40 + 32) + 1 + 15 + 6 + 7


def layer(tokens, cotangent, ids, weights, gate_w, up_w, down_w):
    width = tokens.shape[1]
    model, size = gate_w.shape
    n = model // width
    wide = jax.ShapeDtypeStruct((width, n * size), BF16)
    ANY = pl.BlockSpec(memory_space=pl.ANY)
    return pl.pallas_call(
        layer_kernel,
        out_shape=(
            wide,
            wide,
            wide,
            jax.ShapeDtypeStruct(cotangent.shape, BF16),
            jax.ShapeDtypeStruct(cotangent.shape, BF16),
            jax.ShapeDtypeStruct(ids.shape, F32),
        ),
        in_specs=[VMEM] * 4 + [ANY] * 3,
        out_specs=(VMEM,) * 6,
        scratch_shapes=[
            pltpu.VMEM((model, size), BF16),
            pltpu.VMEM((model, size), BF16),
            pltpu.VMEM((size, model), BF16),
            pltpu.VMEM((size, model), BF16),
            pltpu.VMEM((size, model), BF16),
            pltpu.VMEM((model, size), BF16),
            pltpu.VMEM((ROWS, PACK), BF16),
            pltpu.VMEM((model, PACK), BF16),
            pltpu.VMEM((3, width, WIN), BF16),
            pltpu.VMEM((size, WIN), BF16),
            pltpu.VMEM((size, WIN), BF16),
            pltpu.VMEM((size, WIN), BF16),
            pltpu.VMEM((n * size, 1024), BF16),
            pltpu.VMEM((2, SIDE * SIDE, width, PACK), BF16),
            pltpu.VMEM((SIDE * SIDE, width, PACK), BF16),
            pltpu.VMEM((SIDE * SIDE, width, PACK), BF16),
            pltpu.VMEM((3, SIDE, width // 2, PACK), BF16),
            pltpu.VMEM((3, SIDE, width // 2, PACK), BF16),
            pltpu.VMEM((2, SIDE, width // 2, PACK), BF16),
            pltpu.VMEM((2, 3, width // 2, PACK), BF16),
            pltpu.VMEM((ROWS, width), BF16),
            pltpu.VMEM((ROWS, width), BF16),
            pltpu.VMEM((ROWS, width), BF16),
            pltpu.VMEM((ROWS, width), BF16),
            pltpu.VMEM((10, 8, 128), F32),
            pltpu.SemaphoreType.DMA((3,)),
            pltpu.SemaphoreType.DMA((N_COPIES,)),
            pltpu.SemaphoreType.DMA((N_COPIES,)),
        ],
        compiler_params=pltpu.CompilerParams(
            collective_id=0, has_side_effects=True, vmem_limit_bytes=63 * 2**20
        ),
        name="layer",
    )(tokens, cotangent, ids, weights, gate_w, up_w, down_w)


def body(tokens, cotangent, expert_ids, combine_weights, w_gate, w_up, w_down):
    gate, up, down, mixed, gt, gc = layer(
        tokens, cotangent, expert_ids.T, combine_weights.T, w_gate[0], w_up[0], w_down[0]
    )
    return mixed, gt, gc.T, gate[None], up[None], down.T[None]


def solution(mesh):
    placed = (
        P("ep", "tp"),
        P("ep", "tp"),
        P("ep", None),
        P("ep", None),
        P("ep", None, "tp"),
        P("ep", None, "tp"),
        P("ep", "tp", None),
    )
    return jax.shard_map(
        body,
        mesh=mesh,
        in_specs=placed,
        out_specs=(
            P("ep", "tp"),
            P("ep", "tp"),
            P("ep", None),
            P("ep", "tp", None),
            P("ep", "tp", None),
            P("ep", None, "tp"),
        ),
        check_vma=False,
    )
```

```python
import jax
import jax.numpy as jnp
from jax import lax
from jax.experimental import pallas as pl
from jax.experimental.pallas import tpu as pltpu
from jax.sharding import PartitionSpec as P

SIDE = 4
CAP = 40
HALF = CAP
PAIR = 2 * HALF
GROUPS = 8
ROWS = GROUPS * PAIR
SLOTS = GROUPS * CAP
PACK = 2 * SLOTS
WIN = 384
F32 = jnp.float32
BF16 = jnp.bfloat16
VMEM = pl.BlockSpec(memory_space=pltpu.VMEM)


def dot(a, b, ca, cb):
    return lax.dot_general(a, b, (((ca,), (cb,)), ((), ())), preferred_element_type=F32)


def iota(shape, dim):
    return lax.broadcasted_iota(jnp.int32, shape, dim)


class Grid:
    def __init__(self):
        t = lax.axis_index("tp")
        self.tp = t
        self.c = t % 2
        self.x = (t // 2) % SIDE
        self.y = t // (2 * SIDE)
        self.z = lax.axis_index("ep")

    def at(self, dy, dx, other=False):
        y = (self.y + (dy + SIDE)) % SIDE
        x = (self.x + (dx + SIDE)) % SIDE
        c = 1 - self.c if other else self.c
        return (y * SIDE + x) * 2 + c

    def block(self, h, o1, o2, other=False):
        return self.at(o2, o1, other) if h == 0 else self.at(o1, o2, other)

    def up(self, k):
        return (self.z + k) % GROUPS


class Copies:
    def __init__(self, send, recv):
        self.send, self.recv, self.n, self.ids, self.started = send, recv, 0, {}, []

    def make(self, key, src, dst, to):
        if key not in self.ids:
            self.ids[key] = len(self.ids)
        j = self.ids[key]
        return pltpu.make_async_remote_copy(
            src_ref=src,
            dst_ref=dst,
            send_sem=self.send.at[j],
            recv_sem=self.recv.at[j],
            device_id=to,
            device_id_type=pl.DeviceIdType.MESH,
        )

    def start(self, key, src, dst, to):
        c = self.make(key, src, dst, to)
        c.start()
        self.started.append(c)

    def wait(self, key, dst, to):
        self.make(key, dst, dst, to).wait_recv()

    def finish(self):
        for c in self.started:
            c.wait_send()


def greet(partners):
    barrier = pltpu.get_barrier_semaphore()
    for to in partners:
        pl.semaphore_signal(barrier, inc=1, device_id=to, device_id_type=pl.DeviceIdType.MESH)


def greeted(partners):
    pl.semaphore_wait(pltpu.get_barrier_semaphore(), len(partners))


def gather(g, cp, name, half, part):
    sib = {"tp": g.at(0, 0, True)}
    dirs = (1, -1)

    def nbr(h, axis, d):
        return {"tp": g.block(h, d, 0) if axis == 1 else g.block(h, 0, d)}

    def send(key, h, axis, d, ref):
        cp.start((name, *key), ref, ref, nbr(h, axis, d))

    def got(key, h, axis, d, ref):
        cp.wait((name, *key), ref, nbr(h, axis, d))

    def across(h, o1, o2):
        ref = half(g.block(h, o1, o2), h)
        cp.start((name, "s", h, o1, o2), ref, ref, sib)

    for h in (0, 1):
        for d in dirs:
            send(("p1", h, d), h, 1, d, half(g.tp, h))
    for h in (0, 1):
        for d in dirs:
            send(("p2", h, 0, d), h, 2, d, half(g.tp, h))
    for h in (0, 1):
        across(h, 0, 0)
    for d in dirs:
        for h in (0, 1):
            b = g.block(h, -d, 0)
            got(("p1", h, d), h, 1, -d, half(b, h))
            send(("f1", h, d), h, 1, d, part(b, h, d, 0))
            for e in dirs:
                send(("p2", h, -d, e), h, 2, e, half(b, h))
            across(h, -d, 0)
    for e in dirs:
        for h in (0, 1):
            b = g.block(h, 0, -e)
            got(("p2", h, 0, e), h, 2, -e, half(b, h))
            send(("f2", h, 0, e), h, 2, e, part(b, h, e, 0))
            across(h, 0, -e)
    for h in (0, 1):
        b = g.block(h, 2, 0)
        for d in dirs:
            got(("f1", h, d), h, 1, -d, part(b, h, d, 0))
        for e in dirs:
            send(("p2", h, 2, e), h, 2, e, half(b, h))
        across(h, 2, 0)
    for o1 in (-1, 1):
        for e in dirs:
            for h in (0, 1):
                b = g.block(h, o1, -e)
                got(("p2", h, o1, e), h, 2, -e, half(b, h))
                send(("f2", h, o1, e), h, 2, e, part(b, h, e, o1))
                across(h, o1, -e)
    for h in (0, 1):
        b = g.block(h, 0, 2)
        for e in dirs:
            got(("f2", h, 0, e), h, 2, -e, part(b, h, e, 0))
        across(h, 0, 2)
    for e in dirs:
        for h in (0, 1):
            b = g.block(h, 2, -e)
            got(("p2", h, 2, e), h, 2, -e, half(b, h))
            send(("f2", h, 2, e), h, 2, e, part(b, h, e, 2))
            across(h, 2, -e)
    for o1 in (-1, 1):
        for h in (0, 1):
            b = g.block(h, o1, 2)
            for e in dirs:
                got(("f2", h, o1, e), h, 2, -e, part(b, h, e, o1))
            across(h, o1, 2)
    for h in (0, 1):
        b = g.block(h, 2, 2)
        for e in dirs:
            got(("f2", h, 2, e), h, 2, -e, part(b, h, e, 2))
        across(h, 2, 2)
    for h in (0, 1):
        for o1 in (0, -1, 1, 2):
            for o2 in (0, -1, 1, 2):
                cp.wait((name, "s", h, o1, o2), half(g.block(h, o1, o2, True), h), sib)


def column(row):
    n = row.shape[1]
    eye = iota((n, n), 0) == iota((n, n), 1)
    return jnp.sum(jnp.where(eye, row, jnp.zeros_like(row)), axis=1, keepdims=True)


def as_row(col):
    n = col.shape[0]
    eye = iota((n, n), 0) == iota((n, n), 1)
    return jnp.sum(jnp.where(eye, col, jnp.zeros_like(col)), axis=0, keepdims=True)


def places(ids):
    n = ids[0].shape[0]
    lane = iota((n, 128), 1).astype(F32)
    before = (iota((n, n), 1) < iota((n, n), 0)).astype(BF16)
    hot = [(ids[k] == lane).astype(F32) for k in (0, 1)]
    seen = [dot(before, hot[k].astype(BF16), 1, 0) for k in (0, 1)]
    seen[1] = seen[1] + jnp.sum(hot[0], axis=0, keepdims=True)
    rank = [jnp.sum(seen[k] * hot[k], axis=1, keepdims=True) for k in (0, 1)]
    row = [ids[k] * PAIR + rank[k] for k in (0, 1)]
    lanes = iota((n, ROWS), 1).astype(F32)
    first = [(lanes == row[k]).astype(BF16) for k in (0, 1)]
    second = [(lanes == row[k] + HALF).astype(BF16) for k in (0, 1)]
    return first, second


def fill_packing(pack):
    j = iota((PAIR, 1), 0)
    lane = iota((PAIR, PACK), 1)
    for z in range(GROUPS):
        s = z * CAP + j
        d = s - CAP
        want = jnp.where(j >= CAP, jnp.where(d < 256, d + 384, d + 64), s)
        pack[z * PAIR : (z + 1) * PAIR, :] = (want == lane).astype(F32).astype(BF16)


def to_all_groups(g, cp, src, dst, name):
    for k in range(1, GROUPS):
        to = g.up(k)
        cp.start(
            (name, k),
            src.at[pl.ds(pl.multiple_of(to * PAIR, PAIR), PAIR)],
            dst.at[pl.ds(pl.multiple_of(g.z * PAIR, PAIR), PAIR)],
            {"ep": to},
        )


def from_all_groups(g, cp, dst, name):
    for k in range(1, GROUPS):
        frm = g.up(GROUPS - k)
        cp.wait((name, k), dst.at[pl.ds(pl.multiple_of(frm * PAIR, PAIR), PAIR)], {"ep": frm})


def own_group(g, src, dst):
    mine = pl.ds(pl.multiple_of(g.z * PAIR, PAIR), PAIR)
    dst[mine] = src[mine]


def turned(t):
    return pltpu.roll(t, 64, 1)


def layer_kernel(
    tok_ref, cot_ref, ids_ref, w_ref, gw_hbm, uw_hbm, dw_hbm,
    wide_ref, rows_ref, gc_ref,
    gw, uw, dw, gwt, uwt, dwt, pack, all_ref, wx, wd, hx, gy, uy,
    act, ship, relay, part_ref, sib, chip, far, tmp, near, mid, fin,
    rows, got, rows2, got2, red, local, send, recv,
):
    g = Grid()
    cp = Copies(send, recv)
    sib_dev = {"tp": g.at(0, 0, True)}
    ring = ((0, 1), (0, -1), (0, 2), (1, 0), (-1, 0), (2, 0))
    partners = (
        [sib_dev] + [{"tp": g.at(*o)} for o in ring] + [{"ep": g.up(k)} for k in range(1, GROUPS)]
    )
    greet(partners)
    loads = [
        pltpu.make_async_copy(a, b, local.at[i])
        for i, (a, b) in enumerate(((gw_hbm, gw), (uw_hbm, uw), (dw_hbm, dw)))
    ]
    for c in loads:
        c.start()

    width = tok_ref.shape[1]
    ids = [column(ids_ref[k : k + 1, :].astype(F32)) for k in (0, 1)]
    w = [column(w_ref[k : k + 1, :]) for k in (0, 1)]
    first, second = places(ids)
    cot = cot_ref[...].astype(F32)
    scaled = [(w[k] * cot).astype(BF16) for k in (0, 1)]
    sent = dot(first[0] + first[1], tok_ref[...], 0, 0)
    sent = sent + dot(second[0], scaled[0], 0, 0) + dot(second[1], scaled[1], 0, 0)
    rows[...] = sent.astype(BF16)
    greeted(partners)
    to_all_groups(g, cp, rows, got, "out")
    own_group(g, rows, got)
    fill_packing(pack)
    for c in loads:
        c.wait()
    size = gw.shape[1]
    blocks = gw.shape[0] // width

    def turn(i, _):
        at = pl.ds(pl.multiple_of(i * 256, 256), 256)
        gwt[:, at] = gw[at, :].T
        uwt[:, at] = uw[at, :].T
        dwt[at, :] = dw[:, at].T
        return _

    lax.fori_loop(0, gw.shape[0] // 256, turn, 0)
    from_all_groups(g, cp, got, "out")
    own = dot(got[...], pack[...], 0, 0).astype(BF16)
    all_ref[pl.ds(pl.multiple_of(g.tp * width, width), width), :] = own
    half_w = width // 2

    def half_in(b, h):
        return all_ref.at[pl.ds(pl.multiple_of(b * width + h * half_w, 16), half_w)]

    def part_in(b, h, q, o):
        rng = pl.ds(0, 384) if (q > 0) == (o in (0, 1)) else pl.ds(384, 256)
        return all_ref.at[pl.ds(pl.multiple_of(b * width + h * half_w, 16), half_w), rng]

    gather(g, cp, "in", half_in, part_in)

    hh = size // 2

    def units(h, _):
        r = pl.ds(pl.multiple_of(h * hh, hh), hh)
        gate = dot(gwt[r, :], all_ref[:, :WIN], 1, 0)
        upp = dot(uwt[r, :], all_ref[:, :WIN], 1, 0)
        gh = dot(dw[r, :], all_ref[:, 256:], 1, 0)
        place = jnp.where(h == 0, g.x, g.y)
        lo = iota((hh, 128), 1) < 64
        for i in range(3):
            t = slice(i * 128, (i + 1) * 128)
            gp, u = gate[:, t], upp[:, t]
            d = turned(gh[:, 0:128]) if i == 2 else gh[:, (i + 1) * 128 : (i + 2) * 128]
            s = jax.nn.sigmoid(gp)
            active = gp * s
            hid = active * u
            gg = d * u * (s * (1.0 + gp * (1.0 - s)))
            gu = d * active
            if i == 2:
                hid, gg, gu = (jnp.where(lo, a, 0.0) for a in (hid, gg, gu))
                act[h, place, g.c, :, 256:384] = (gg + turned(hid)).astype(BF16)
                gy[r, 0:128] = turned(gg).astype(BF16)
                uy[r, 0:128] = turned(gu).astype(BF16)
            else:
                act[h, place, g.c, :, t] = gg.astype(BF16)
                act[h, place, g.c, :, 384 + i * 128 : 512 + i * 128] = hid.astype(BF16)
                gy[r, (i + 1) * 128 : (i + 2) * 128] = gg.astype(BF16)
                uy[r, (i + 1) * 128 : (i + 2) * 128] = gu.astype(BF16)
            hx[r, t] = hid.astype(BF16)
            act[h, place, g.c, :, 640 + i * 128 : 768 + i * 128] = gu.astype(BF16)
        return _

    lax.fori_loop(0, 2, units, 0)

    dirs = (1, -1)
    dests = (0, 1, -1, 2)
    lines = (0, -1, 1, 2)

    def spot(h, o1):
        return ((g.x if h == 0 else g.y) + (o1 + SIDE)) % SIDE

    def nbr(h, axis, d):
        return {"tp": g.block(h, d, 0) if axis == 1 else g.block(h, 0, d)}

    def piece(h, o1, d):
        return act.at[h, spot(h, o1), g.c, pl.ds(0 if d > 0 else hh // 2, hh // 2)]

    def cross(h, o1):
        ref = act.at[h, spot(h, o1), g.c]
        cp.start(("s", h, o1), ref, ref, sib_dev)

    def crossed(h, o1):
        cp.wait(("s", h, o1), act.at[h, spot(h, o1), 1 - g.c], sib_dev)

    def columns(h, o1, o2, k):
        b = g.block(h, o1, o2, k == 1)
        return pl.ds(pl.multiple_of(b * size + h * hh, 128), hh)

    def make(h, o1, k):
        j = lines.index(o1)
        c = g.c if k == 0 else 1 - g.c
        blk = act[h, spot(h, o1), c]
        for i, (left, right) in enumerate(
            ((wx[h], blk[:, :WIN]), (wx[h], blk[:, 640:]), (wd[h], blk[:, 256:640]))
        ):
            res = dot(left, right, 1, 1).astype(BF16)
            wide_ref[i, :, columns(h, o1, 0, k)] = res[0:width]
            for n in range(3):
                ship[h, j, k, n, i] = res[(n + 1) * width : (n + 2) * width]
        for n, d in enumerate(dirs):
            cp.start(
                ("w", h, o1, k, d), ship.at[h, j, k, n], wide_ref.at[:, :, columns(h, o1, 0, k)], nbr(h, 2, d)
            )
        d = dirs[k]
        cp.start(("v", h, o1, d), ship.at[h, j, k, 2], relay.at[h, j, k], nbr(h, 2, d))

    def pass_on(h, o1):
        j = lines.index(o1)
        for k, d in enumerate(dirs):
            cp.wait(("v", h, o1, d), relay.at[h, j, k], nbr(h, 2, -d))
            cp.start(
                ("u", h, o1, d), relay.at[h, j, k], wide_ref.at[:, :, columns(h, o1, -d, k)], nbr(h, 2, d)
            )

    def landed(h, o1):
        for k, d in enumerate(dirs):
            for e in dirs:
                cp.wait(("w", h, o1, k, e), wide_ref.at[:, :, columns(h, o1, -e, k)], nbr(h, 2, -e))
            cp.wait(("u", h, o1, d), wide_ref.at[:, :, columns(h, o1, 2, k)], nbr(h, 2, -d))

    for h in (0, 1):
        ref = act.at[h, spot(h, 0), g.c]
        for d in dirs:
            cp.start(("p", h, d), ref, ref, nbr(h, 1, d))
        cross(h, 0)
    low = iota((width, 128), 1) < 64
    for h in (0, 1):
        for n, o2 in enumerate(dests):
            at = pl.ds(pl.multiple_of(g.block(h, 0, o2) * width, width), width)
            r = pl.ds(n * width, width)
            shared = all_ref[at, 256:384].astype(F32)
            wx[h, r, 0:256] = all_ref[at, 0:256]
            wx[h, r, 256:384] = jnp.where(low, shared, 0.0).astype(BF16)
            wd[h, r, 0:128] = jnp.where(low, 0.0, shared).astype(BF16)
            wd[h, r, 128:384] = all_ref[at, 384:640]
    for h in (0, 1):
        make(h, 0, 0)
    for h in (0, 1):
        crossed(h, 0)
        make(h, 0, 1)

    def partial(c):
        def one(i, _):
            at = pl.ds(pl.multiple_of((2 * i + c) * width, width), width)
            out = dot(dwt[at, :], hx[...], 1, 0)
            inn = dot(gw[at, :], gy[...], 1, 0) + dot(uw[at, :], uy[...], 1, 0)
            part_ref[c, i, :, 0:256] = out[:, 0:256].astype(BF16)
            part_ref[c, i, :, 256:384] = (out[:, 256:] + inn[:, :128]).astype(BF16)
            part_ref[c, i, :, 384:640] = inn[:, 128:].astype(BF16)
            return _

        lax.fori_loop(0, blocks // 2, one, 0)

    partial(1 - g.c)
    cp.start("pair", part_ref.at[1 - g.c], sib, sib_dev)
    partial(g.c)
    cp.wait("pair", sib, sib_dev)

    def add_pair(i, _):
        chip[i // SIDE, i % SIDE] = (part_ref[g.c, i].astype(F32) + sib[i].astype(F32)).astype(BF16)
        return _

    lax.fori_loop(0, SIDE * SIDE, add_pair, 0)

    def y_of(d):
        return (g.y + d + SIDE) % SIDE

    def x_of(d):
        return (g.x + d + SIDE) % SIDE

    rng = (pl.ds(0, half_w), pl.ds(half_w, half_w))

    def share(h, d, q):
        two = pl.ds(2 * q, 2)
        return (y_of(d), two, rng[0]) if h == 0 else (two, x_of(d), rng[1])

    for h in (0, 1):
        for q, d in enumerate(dirs):
            cp.start(("r1", h, d), chip.at[share(h, 2, q)], far.at[h, q], nbr(h, 2, d))
        for q, d in enumerate(dirs):
            cp.start(("r2", h, d), chip.at[share(h, d, 1 - q)], near.at[h, q, 1], nbr(h, 2, d))
    for q, d in enumerate(dirs):
        for h in (0, 1):
            cp.wait(("r1", h, d), far.at[h, q], nbr(h, 2, -d))
            tmp[h, q] = (chip[share(h, d, q)].astype(F32) + far[h, q].astype(F32)).astype(BF16)
            cp.start(("r3", h, d), tmp.at[h, q], near.at[h, q, 0], nbr(h, 2, d))
    for d in dirs:
        for h in (0, 1):
            cp.wait(("p", h, d), act.at[h, spot(h, -d), g.c], nbr(h, 1, -d))
            cp.start(("f", h, d), piece(h, -d, d), piece(h, -d, d), nbr(h, 1, d))
            cross(h, -d)
    for h in (0, 1):
        pass_on(h, 0)
    for d in dirs:
        for h in (0, 1):
            make(h, -d, 0)
    for h in (0, 1):
        for q, d in enumerate(dirs):
            cp.wait(("r2", h, d), near.at[h, q, 1], nbr(h, 2, -d))
            cp.wait(("r3", h, d), near.at[h, q, 0], nbr(h, 2, -d))
        for q in (0, 1):
            t = chip[share(h, 0, q)].astype(F32)
            t = t + near[h, q, 0].astype(F32) + near[h, 1 - q, 1].astype(F32)
            mid[h, 2 * q : 2 * q + 2] = t.astype(BF16)
    for i, d in enumerate((1, -1, 2)):
        cp.start(("a2", d), mid.at[0, x_of(d)], fin.at[0, i], {"tp": g.at(0, d)})
        cp.start(("b2", d), mid.at[1, y_of(d)], fin.at[1, i], {"tp": g.at(d, 0)})
    for d in dirs:
        for h in (0, 1):
            crossed(h, -d)
            make(h, -d, 1)
    for i, d in enumerate((1, -1, 2)):
        cp.wait(("a2", d), fin.at[0, i], {"tp": g.at(0, -d)})
        cp.wait(("b2", d), fin.at[1, i], {"tp": g.at(-d, 0)})
    sums = []
    for h in (0, 1):
        s = mid[h, g.x if h == 0 else g.y].astype(F32)
        for i in range(3):
            s = s + fin[h, i].astype(F32)
        sums.append(s)
    total = jnp.concatenate(sums, axis=0).astype(BF16)
    rows2[...] = dot(pack[...], total, 1, 1).astype(BF16)
    to_all_groups(g, cp, rows2, got2, "back")
    own_group(g, rows2, got2)
    for h in (0, 1):
        for d in dirs:
            cp.wait(("f", h, d), piece(h, 2, d), nbr(h, 1, -d))
        cross(h, 2)
        make(h, 2, 0)
    for h in (0, 1):
        crossed(h, 2)
        make(h, 2, 1)
        for o1 in (-1, 1):
            pass_on(h, o1)
    from_all_groups(g, cp, got2, "back")
    back = got2[...]
    outs = [dot(first[k], back, 1, 0) for k in (0, 1)]
    rows_ref[0] = (w[0] * outs[0] + w[1] * outs[1]).astype(BF16)
    rows_ref[1] = (dot(second[0], back, 1, 0) + dot(second[1], back, 1, 0)).astype(BF16)
    inner = [as_row(jnp.sum(cot * outs[k], axis=1, keepdims=True)) for k in (0, 1)]
    sub = iota((8, width), 0)
    red[0] = jnp.zeros((8, 128), F32)
    red[0, :, 0:width] = jnp.where(sub == 0, inner[0], jnp.where(sub == 1, inner[1], 0.0))
    cp.start("g0", red.at[0], red.at[1], sib_dev)
    for h in (0, 1):
        pass_on(h, 2)
    cp.wait("g0", red.at[1], sib_dev)
    red[2 + g.x] = red[0] + red[1]
    for d in (1, -1, 2):
        cp.start(("g1", d), red.at[2 + g.x], red.at[2 + g.x], {"tp": g.at(0, d)})
    for h in (0, 1):
        landed(h, 0)
    for d in (1, -1, 2):
        cp.wait(("g1", d), red.at[2 + x_of(-d)], {"tp": g.at(0, -d)})
    red[6 + g.y] = (red[2] + red[3]) + (red[4] + red[5])
    for d in (1, -1, 2):
        cp.start(("g2", d), red.at[6 + g.y], red.at[6 + g.y], {"tp": g.at(d, 0)})
    for h in (0, 1):
        for o1 in (-1, 1, 2):
            landed(h, o1)
    for d in (1, -1, 2):
        cp.wait(("g2", d), red.at[6 + y_of(-d)], {"tp": g.at(-d, 0)})
    gc_ref[...] = ((red[6] + red[7]) + (red[8] + red[9]))[0:2, 0:width]
    cp.finish()


N_COPIES = 2 * 7 + (40 + 32) + (4 + 4 + 8 + 32 + 16 + 16) + 1 + 12 + 6 + 7


def layer(tokens, cotangent, ids, weights, gate_w, up_w, down_w):
    width = tokens.shape[1]
    model, size = gate_w.shape
    n = model // width
    ANY = pl.BlockSpec(memory_space=pl.ANY)
    half_w = width // 2
    return pl.pallas_call(
        layer_kernel,
        out_shape=(
            pltpu.VMEM((3, width, n * size), BF16),
                        pltpu.VMEM((2, *cotangent.shape), BF16),
            pltpu.VMEM(ids.shape, F32),
        ),
        in_specs=[VMEM] * 4 + [ANY] * 3,
        out_specs=(VMEM,) * 3,
        scratch_shapes=[
            pltpu.VMEM((model, size), BF16),
            pltpu.VMEM((model, size), BF16),
            pltpu.VMEM((size, model), BF16),
            pltpu.VMEM((size, model), BF16),
            pltpu.VMEM((size, model), BF16),
            pltpu.VMEM((model, size), BF16),
            pltpu.VMEM((ROWS, PACK), BF16),
            pltpu.VMEM((model, PACK), BF16),
            pltpu.VMEM((2, SIDE * width, WIN), BF16),
            pltpu.VMEM((2, SIDE * width, WIN), BF16),
            pltpu.VMEM((size, WIN), BF16),
            pltpu.VMEM((size, WIN), BF16),
            pltpu.VMEM((size, WIN), BF16),
            pltpu.VMEM((2, SIDE, 2, size // 2, 1024), BF16),
            pltpu.VMEM((2, SIDE, 2, 3, 3, width, size // 2), BF16),
            pltpu.VMEM((2, SIDE, 2, 3, width, size // 2), BF16),
            pltpu.VMEM((2, SIDE * SIDE, width, PACK), BF16),
            pltpu.VMEM((SIDE * SIDE, width, PACK), BF16),
            pltpu.VMEM((SIDE, SIDE, width, PACK), BF16),
            pltpu.VMEM((2, 2, 2, half_w, PACK), BF16),
            pltpu.VMEM((2, 2, 2, half_w, PACK), BF16),
            pltpu.VMEM((2, 2, 2, 2, half_w, PACK), BF16),
            pltpu.VMEM((2, SIDE, half_w, PACK), BF16),
            pltpu.VMEM((2, 3, half_w, PACK), BF16),
            pltpu.VMEM((ROWS, width), BF16),
            pltpu.VMEM((ROWS, width), BF16),
            pltpu.VMEM((ROWS, width), BF16),
            pltpu.VMEM((ROWS, width), BF16),
            pltpu.VMEM((10, 8, 128), F32),
            pltpu.SemaphoreType.DMA((3,)),
            pltpu.SemaphoreType.DMA((N_COPIES,)),
            pltpu.SemaphoreType.DMA((N_COPIES,)),
        ],
        compiler_params=pltpu.CompilerParams(
            collective_id=0, has_side_effects=True, vmem_limit_bytes=52 * 2**20
        ),
        name="layer",
    )(tokens, cotangent, ids, weights, gate_w, up_w, down_w)


def body(tokens, cotangent, expert_ids, combine_weights, w_gate, w_up, w_down):
    wide, back, gc = layer(
        tokens, cotangent, expert_ids.T, combine_weights.T, w_gate[0], w_up[0], w_down[0]
    )
    return back[0], back[1], gc.T, wide[0][None], wide[1][None], wide[2].T[None]


def solution(mesh):
    placed = (
        P("ep", "tp"),
        P("ep", "tp"),
        P("ep", None),
        P("ep", None),
        P("ep", None, "tp"),
        P("ep", None, "tp"),
        P("ep", "tp", None),
    )
    return jax.shard_map(
        body,
        mesh=mesh,
        in_specs=placed,
        out_specs=(
            P("ep", "tp"),
            P("ep", "tp"),
            P("ep", None),
            P("ep", "tp", None),
            P("ep", "tp", None),
            P("ep", None, "tp"),
        ),
        check_vma=False,
    )
```

```python
import jax
import jax.numpy as jnp
from jax import lax
from jax.experimental import pallas as pl
from jax.experimental.pallas import tpu as pltpu
from jax.sharding import PartitionSpec as P

SIDE = 4
CAP = 40
HALF = CAP
PAIR = 2 * HALF
GROUPS = 8
ROWS = GROUPS * PAIR
SLOTS = GROUPS * CAP
PACK = 2 * SLOTS
WIN = 384
F32 = jnp.float32
BF16 = jnp.bfloat16
VMEM = pl.BlockSpec(memory_space=pltpu.VMEM)


def dot(a, b, ca, cb):
    return lax.dot_general(a, b, (((ca,), (cb,)), ((), ())), preferred_element_type=F32)


def iota(shape, dim):
    return lax.broadcasted_iota(jnp.int32, shape, dim)


class Grid:
    def __init__(self):
        t = lax.axis_index("tp")
        self.tp = t
        self.c = t % 2
        self.x = (t // 2) % SIDE
        self.y = t // (2 * SIDE)
        self.z = lax.axis_index("ep")

    def at(self, dy, dx, other=False):
        y = (self.y + (dy + SIDE)) % SIDE
        x = (self.x + (dx + SIDE)) % SIDE
        c = 1 - self.c if other else self.c
        return (y * SIDE + x) * 2 + c

    def block(self, h, o1, o2, other=False):
        return self.at(o2, o1, other) if h == 0 else self.at(o1, o2, other)

    def up(self, k):
        return (self.z + k) % GROUPS


class Copies:
    def __init__(self, send, recv):
        self.send, self.recv, self.n, self.ids, self.started = send, recv, 0, {}, []

    def make(self, key, src, dst, to):
        if key not in self.ids:
            self.ids[key] = len(self.ids)
        j = self.ids[key]
        return pltpu.make_async_remote_copy(
            src_ref=src,
            dst_ref=dst,
            send_sem=self.send.at[j],
            recv_sem=self.recv.at[j],
            device_id=to,
            device_id_type=pl.DeviceIdType.MESH,
        )

    def start(self, key, src, dst, to):
        c = self.make(key, src, dst, to)
        c.start()
        self.started.append(c)

    def wait(self, key, dst, to):
        self.make(key, dst, dst, to).wait_recv()

    def finish(self):
        for c in self.started:
            c.wait_send()


def greet(partners):
    barrier = pltpu.get_barrier_semaphore()
    for to in partners:
        pl.semaphore_signal(barrier, inc=1, device_id=to, device_id_type=pl.DeviceIdType.MESH)


def greeted(partners):
    pl.semaphore_wait(pltpu.get_barrier_semaphore(), len(partners))


def gather(g, cp, name, half, part):
    sib = {"tp": g.at(0, 0, True)}
    dirs = (1, -1)

    def nbr(h, axis, d):
        return {"tp": g.block(h, d, 0) if axis == 1 else g.block(h, 0, d)}

    def send(key, h, axis, d, ref):
        cp.start((name, *key), ref, ref, nbr(h, axis, d))

    def got(key, h, axis, d, ref):
        cp.wait((name, *key), ref, nbr(h, axis, d))

    def across(h, o1, o2):
        ref = half(g.block(h, o1, o2), h)
        cp.start((name, "s", h, o1, o2), ref, ref, sib)

    for h in (0, 1):
        for d in dirs + (2,):
            send(("p1", h, d), h, 1, d, half(g.tp, h))
    for h in (0, 1):
        for d in dirs:
            send(("p2", h, 0, d), h, 2, d, half(g.tp, h))
    for h in (0, 1):
        across(h, 0, 0)
    for d in dirs:
        for h in (0, 1):
            b = g.block(h, -d, 0)
            got(("p1", h, d), h, 1, -d, half(b, h))
            for e in dirs:
                send(("p2", h, -d, e), h, 2, e, half(b, h))
            across(h, -d, 0)
    for h in (0, 1):
        b = g.block(h, 2, 0)
        got(("p1", h, 2), h, 1, 2, half(b, h))
        for e in dirs + (2,):
            send(("p2", h, 2, e), h, 2, e, half(b, h))
        across(h, 2, 0)
    for e in dirs:
        for h in (0, 1):
            b = g.block(h, 0, -e)
            got(("p2", h, 0, e), h, 2, -e, half(b, h))
            send(("f2", h, 0, e), h, 2, e, part(b, h, e, 0))
            across(h, 0, -e)
    for o1 in (-1, 1):
        for e in dirs:
            for h in (0, 1):
                b = g.block(h, o1, -e)
                got(("p2", h, o1, e), h, 2, -e, half(b, h))
                send(("f2", h, o1, e), h, 2, e, part(b, h, e, o1))
                across(h, o1, -e)
    for h in (0, 1):
        b = g.block(h, 0, 2)
        for e in dirs:
            got(("f2", h, 0, e), h, 2, -e, part(b, h, e, 0))
        across(h, 0, 2)
    for e in dirs:
        for h in (0, 1):
            b = g.block(h, 2, -e)
            got(("p2", h, 2, e), h, 2, -e, half(b, h))
            across(h, 2, -e)
    for o1 in (-1, 1):
        for h in (0, 1):
            b = g.block(h, o1, 2)
            for e in dirs:
                got(("f2", h, o1, e), h, 2, -e, part(b, h, e, o1))
            across(h, o1, 2)
    for h in (0, 1):
        b = g.block(h, 2, 2)
        got(("p2", h, 2, 2), h, 2, 2, half(b, h))
        across(h, 2, 2)
    for h in (0, 1):
        for o1 in (0, -1, 1, 2):
            for o2 in (0, -1, 1, 2):
                cp.wait((name, "s", h, o1, o2), half(g.block(h, o1, o2, True), h), sib)


def column(row):
    n = row.shape[1]
    eye = iota((n, n), 0) == iota((n, n), 1)
    return jnp.sum(jnp.where(eye, row, jnp.zeros_like(row)), axis=1, keepdims=True)


def as_row(col):
    n = col.shape[0]
    eye = iota((n, n), 0) == iota((n, n), 1)
    return jnp.sum(jnp.where(eye, col, jnp.zeros_like(col)), axis=0, keepdims=True)


def places(ids):
    n = ids[0].shape[0]
    lane = iota((n, 128), 1).astype(F32)
    before = (iota((n, n), 1) < iota((n, n), 0)).astype(BF16)
    hot = [(ids[k] == lane).astype(F32) for k in (0, 1)]
    seen = [dot(before, hot[k].astype(BF16), 1, 0) for k in (0, 1)]
    seen[1] = seen[1] + jnp.sum(hot[0], axis=0, keepdims=True)
    rank = [jnp.sum(seen[k] * hot[k], axis=1, keepdims=True) for k in (0, 1)]
    row = [ids[k] * PAIR + rank[k] for k in (0, 1)]
    lanes = iota((n, ROWS), 1).astype(F32)
    first = [(lanes == row[k]).astype(BF16) for k in (0, 1)]
    second = [(lanes == row[k] + HALF).astype(BF16) for k in (0, 1)]
    return first, second


def fill_packing(pack):
    j = iota((PAIR, 1), 0)
    lane = iota((PAIR, PACK), 1)
    for z in range(GROUPS):
        s = z * CAP + j
        d = s - CAP
        want = jnp.where(j >= CAP, jnp.where(d < 256, d + 384, d + 64), s)
        pack[z * PAIR : (z + 1) * PAIR, :] = (want == lane).astype(F32).astype(BF16)


def to_all_groups(g, cp, src, dst, name):
    for k in range(1, GROUPS):
        to = g.up(k)
        cp.start(
            (name, k),
            src.at[pl.ds(pl.multiple_of(to * PAIR, PAIR), PAIR)],
            dst.at[pl.ds(pl.multiple_of(g.z * PAIR, PAIR), PAIR)],
            {"ep": to},
        )


def from_all_groups(g, cp, dst, name):
    for k in range(1, GROUPS):
        frm = g.up(GROUPS - k)
        cp.wait((name, k), dst.at[pl.ds(pl.multiple_of(frm * PAIR, PAIR), PAIR)], {"ep": frm})


def own_group(g, src, dst):
    mine = pl.ds(pl.multiple_of(g.z * PAIR, PAIR), PAIR)
    dst[mine] = src[mine]


def turned(t):
    return pltpu.roll(t, 64, 1)


def layer_kernel(
    tok_hbm, cot_hbm, ids_hbm, w_hbm, gw_hbm, uw_hbm, dw_hbm,
    wide_ref, rows_ref, gc_ref,
    tok_ref, cot_ref, ids_ref, w_ref,
    gw, uw, dw, gwt, uwt, dwt, pack, all_ref, wx, wd, hx, gy, uy,
    act, ship, relay, part_ref, sib, chip, far, tmp, near, mid, fin,
    rows, got, rows2, got2, red, local, send, recv,
):
    g = Grid()
    cp = Copies(send, recv)
    sib_dev = {"tp": g.at(0, 0, True)}
    ring = ((0, 1), (0, -1), (0, 2), (1, 0), (-1, 0), (2, 0))
    others = ((0, 1, True), (0, -1, True), (0, 2, True))
    partners = (
        [sib_dev] + [{"tp": g.at(*o)} for o in ring + others] + [{"ep": g.up(k)} for k in range(1, GROUPS)]
    )
    greet(partners)
    loads = [
        pltpu.make_async_copy(a, b, local.at[i])
        for i, (a, b) in enumerate(
            (
                (tok_hbm, tok_ref),
                (cot_hbm, cot_ref),
                (ids_hbm, ids_ref),
                (w_hbm, w_ref),
                (gw_hbm, gw),
                (uw_hbm, uw),
                (dw_hbm, dw),
            )
        )
    ]
    for c in loads:
        c.start()
    for c in loads[:4]:
        c.wait()

    width = tok_ref.shape[1]
    ids = [column(ids_ref[k : k + 1, :].astype(F32)) for k in (0, 1)]
    w = [column(w_ref[k : k + 1, :]) for k in (0, 1)]
    first, second = places(ids)
    cot = cot_ref[...].astype(F32)
    scaled = [(w[k] * cot).astype(BF16) for k in (0, 1)]
    sent = dot(first[0] + first[1], tok_ref[...], 0, 0)
    sent = sent + dot(second[0], scaled[0], 0, 0) + dot(second[1], scaled[1], 0, 0)
    rows[...] = sent.astype(BF16)
    greeted(partners)
    to_all_groups(g, cp, rows, got, "out")
    own_group(g, rows, got)
    fill_packing(pack)
    for c in loads[4:]:
        c.wait()
    size = gw.shape[1]
    blocks = gw.shape[0] // width

    def turn(i, _):
        at = pl.ds(pl.multiple_of(i * 256, 256), 256)
        gwt[:, at] = gw[at, :].T
        uwt[:, at] = uw[at, :].T
        dwt[at, :] = dw[:, at].T
        return _

    lax.fori_loop(0, gw.shape[0] // 256, turn, 0)
    from_all_groups(g, cp, got, "out")
    own = dot(got[...], pack[...], 0, 0).astype(BF16)
    all_ref[pl.ds(pl.multiple_of(g.tp * width, width), width), :] = own
    half_w = width // 2

    def half_in(b, h):
        return all_ref.at[pl.ds(pl.multiple_of(b * width + h * half_w, 16), half_w)]

    def part_in(b, h, q, o):
        rng = pl.ds(0, 384) if (q > 0) == (o in (0, 1)) else pl.ds(384, 256)
        return all_ref.at[pl.ds(pl.multiple_of(b * width + h * half_w, 16), half_w), rng]

    gather(g, cp, "in", half_in, part_in)

    hh = size // 2

    def units(h, _):
        r = pl.ds(h * hh, hh)
        gate = dot(gwt[r, :], all_ref[:, :WIN], 1, 0)
        upp = dot(uwt[r, :], all_ref[:, :WIN], 1, 0)
        gh = dot(dw[r, :], all_ref[:, 256:], 1, 0)
        place = g.x if h == 0 else g.y
        lo = iota((hh, 128), 1) < 64
        for i in range(3):
            t = slice(i * 128, (i + 1) * 128)
            gp, u = gate[:, t], upp[:, t]
            d = turned(gh[:, 0:128]) if i == 2 else gh[:, (i + 1) * 128 : (i + 2) * 128]
            s = jax.nn.sigmoid(gp)
            active = gp * s
            hid = active * u
            gg = d * u * (s * (1.0 + gp * (1.0 - s)))
            gu = d * active
            if i == 2:
                hid, gg, gu = (jnp.where(lo, a, 0.0) for a in (hid, gg, gu))
                act[h, place, g.c, :, 256:384] = (gg + turned(hid)).astype(BF16)
                gy[r, 0:128] = turned(gg).astype(BF16)
                uy[r, 0:128] = turned(gu).astype(BF16)
            else:
                act[h, place, g.c, :, t] = gg.astype(BF16)
                act[h, place, g.c, :, 384 + i * 128 : 512 + i * 128] = hid.astype(BF16)
                gy[r, (i + 1) * 128 : (i + 2) * 128] = gg.astype(BF16)
                uy[r, (i + 1) * 128 : (i + 2) * 128] = gu.astype(BF16)
            hx[r, t] = hid.astype(BF16)
            act[h, place, g.c, :, 640 + i * 128 : 768 + i * 128] = gu.astype(BF16)
        return _


    dirs = (1, -1)
    dests = (0, 1, -1, 2)
    lines = (0, -1, 1, 2)

    def spot(h, o1):
        return ((g.x if h == 0 else g.y) + (o1 + SIDE)) % SIDE

    def nbr(h, axis, d):
        return {"tp": g.block(h, d, 0) if axis == 1 else g.block(h, 0, d)}

    def piece(h, o1, d):
        return act.at[h, spot(h, o1), g.c, pl.ds(0 if d > 0 else hh // 2, hh // 2)]

    def cross(h, o1):
        ref = act.at[h, spot(h, o1), g.c]
        cp.start(("s", h, o1), ref, ref, sib_dev)

    def crossed(h, o1):
        cp.wait(("s", h, o1), act.at[h, spot(h, o1), 1 - g.c], sib_dev)

    def columns(h, o1, o2, k):
        b = g.block(h, o1, o2, k == 1)
        return pl.ds(pl.multiple_of(b * size + h * hh, 128), hh)

    def make(h, o1, k):
        j = lines.index(o1)
        c = g.c if k == 0 else 1 - g.c
        blk = act[h, spot(h, o1), c]
        for i, (left, right) in enumerate(
            ((wx[h], blk[:, :WIN]), (wx[h], blk[:, 640:]), (wd[h], blk[:, 256:640]))
        ):
            res = dot(left, right, 1, 1).astype(BF16)
            wide_ref[i, :, columns(h, o1, 0, k)] = res[0:width]
            for n in range(3):
                ship[h, j, k, n, i] = res[(n + 1) * width : (n + 2) * width]
        for n, d in enumerate(dirs):
            cp.start(
                ("w", h, o1, k, d), ship.at[h, j, k, n], wide_ref.at[:, :, columns(h, o1, 0, k)], nbr(h, 2, d)
            )
        d = dirs[k]
        cp.start(("v", h, o1, d), ship.at[h, j, k, 2], relay.at[h, j, k], nbr(h, 2, d))

    def pass_on(h, o1):
        j = lines.index(o1)
        for k, d in enumerate(dirs):
            cp.wait(("v", h, o1, d), relay.at[h, j, k], nbr(h, 2, -d))
            cp.start(
                ("u", h, o1, d), relay.at[h, j, k], wide_ref.at[:, :, columns(h, o1, -d, k)], nbr(h, 2, d)
            )

    def landed(h, o1):
        for k, d in enumerate(dirs):
            for e in dirs:
                cp.wait(("w", h, o1, k, e), wide_ref.at[:, :, columns(h, o1, -e, k)], nbr(h, 2, -e))
            cp.wait(("u", h, o1, d), wide_ref.at[:, :, columns(h, o1, 2, k)], nbr(h, 2, -d))

    for h in (0, 1):
        units(h, 0)
        ref = act.at[h, spot(h, 0), g.c]
        for d in dirs:
            cp.start(("p", h, d), ref, ref, nbr(h, 1, d))
        cross(h, 0)
    low = iota((width, 128), 1) < 64
    for h in (0, 1):
        for n, o2 in enumerate(dests):
            at = pl.ds(pl.multiple_of(g.block(h, 0, o2) * width, width), width)
            r = pl.ds(n * width, width)
            shared = all_ref[at, 256:384].astype(F32)
            wx[h, r, 0:256] = all_ref[at, 0:256]
            wx[h, r, 256:384] = jnp.where(low, shared, 0.0).astype(BF16)
            wd[h, r, 0:128] = jnp.where(low, 0.0, shared).astype(BF16)
            wd[h, r, 128:384] = all_ref[at, 384:640]
    for h in (0, 1):
        make(h, 0, 0)
    for h in (0, 1):
        crossed(h, 0)
        make(h, 0, 1)

    def partial(c):
        def one(i, _):
            at = pl.ds(pl.multiple_of((2 * i + c) * width, width), width)
            out = dot(dwt[at, :], hx[...], 1, 0)
            inn = dot(gw[at, :], gy[...], 1, 0) + dot(uw[at, :], uy[...], 1, 0)
            part_ref[c, i, :, 0:256] = out[:, 0:256].astype(BF16)
            part_ref[c, i, :, 256:384] = (out[:, 256:] + inn[:, :128]).astype(BF16)
            part_ref[c, i, :, 384:640] = inn[:, 128:].astype(BF16)
            return _

        lax.fori_loop(0, blocks // 2, one, 0)

    partial(1 - g.c)
    cp.start("pair", part_ref.at[1 - g.c], sib, sib_dev)
    partial(g.c)
    cp.wait("pair", sib, sib_dev)

    def add_pair(i, _):
        chip[i // SIDE, i % SIDE] = (part_ref[g.c, i].astype(F32) + sib[i].astype(F32)).astype(BF16)
        return _

    lax.fori_loop(0, SIDE * SIDE, add_pair, 0)

    def y_of(d):
        return (g.y + d + SIDE) % SIDE

    def x_of(d):
        return (g.x + d + SIDE) % SIDE

    rng = (pl.ds(0, half_w), pl.ds(half_w, half_w))

    def share(h, d, q):
        two = pl.ds(2 * q, 2)
        return (y_of(d), two, rng[0]) if h == 0 else (two, x_of(d), rng[1])

    for h in (0, 1):
        for q, d in enumerate(dirs):
            cp.start(("r1", h, d), chip.at[share(h, 2, q)], far.at[h, q], nbr(h, 2, d))
        for q, d in enumerate(dirs):
            cp.start(("r2", h, d), chip.at[share(h, d, 1 - q)], near.at[h, q, 1], nbr(h, 2, d))
    for q, d in enumerate(dirs):
        for h in (0, 1):
            cp.wait(("r1", h, d), far.at[h, q], nbr(h, 2, -d))
            tmp[h, q] = (chip[share(h, d, q)].astype(F32) + far[h, q].astype(F32)).astype(BF16)
            cp.start(("r3", h, d), tmp.at[h, q], near.at[h, q, 0], nbr(h, 2, d))
    for d in dirs:
        for h in (0, 1):
            cp.wait(("p", h, d), act.at[h, spot(h, -d), g.c], nbr(h, 1, -d))
            cp.start(("f", h, d), piece(h, -d, d), piece(h, -d, d), nbr(h, 1, d))
            cross(h, -d)
    for h in (0, 1):
        pass_on(h, 0)
    for d in dirs:
        for h in (0, 1):
            make(h, -d, 0)
    for h in (0, 1):
        for q, d in enumerate(dirs):
            cp.wait(("r2", h, d), near.at[h, q, 1], nbr(h, 2, -d))
            cp.wait(("r3", h, d), near.at[h, q, 0], nbr(h, 2, -d))
        for q in (0, 1):
            t = chip[share(h, 0, q)].astype(F32)
            t = t + near[h, q, 0].astype(F32) + near[h, 1 - q, 1].astype(F32)
            mid[h, 2 * q : 2 * q + 2] = t.astype(BF16)
    for i, d in enumerate((1, -1, 2)):
        cp.start(("a2", d), mid.at[0, x_of(d)], fin.at[0, i], {"tp": g.at(0, d)})
        cp.start(("b2", d), mid.at[1, y_of(d)], fin.at[1, i], {"tp": g.at(d, 0)})
    for d in dirs:
        for h in (0, 1):
            crossed(h, -d)
            make(h, -d, 1)
    for h in (0, 1):
        for d in dirs:
            cp.wait(("f", h, d), piece(h, 2, d), nbr(h, 1, -d))
        cross(h, 2)
        make(h, 2, 0)
    for h in (0, 1):
        crossed(h, 2)
        make(h, 2, 1)
    for i, d in enumerate((1, -1, 2)):
        cp.wait(("a2", d), fin.at[0, i], {"tp": g.at(0, -d)})
        cp.wait(("b2", d), fin.at[1, i], {"tp": g.at(-d, 0)})
    sums = []
    for h in (0, 1):
        s = mid[h, g.x if h == 0 else g.y].astype(F32)
        for i in range(3):
            s = s + fin[h, i].astype(F32)
        sums.append(s)
    total = jnp.concatenate(sums, axis=0).astype(BF16)
    rows2[...] = dot(pack[...], total, 1, 1).astype(BF16)
    to_all_groups(g, cp, rows2, got2, "back")
    own_group(g, rows2, got2)
    for h in (0, 1):
        for o1 in (-1, 1):
            pass_on(h, o1)
    from_all_groups(g, cp, got2, "back")
    back = got2[...]
    outs = [dot(first[k], back, 1, 0) for k in (0, 1)]
    rows_ref[0] = (w[0] * outs[0] + w[1] * outs[1]).astype(BF16)
    rows_ref[1] = (dot(second[0], back, 1, 0) + dot(second[1], back, 1, 0)).astype(BF16)
    inner = [as_row(jnp.sum(cot * outs[k], axis=1, keepdims=True)) for k in (0, 1)]
    sub = iota((8, width), 0)
    red[2 * g.x + g.c] = jnp.zeros((8, 128), F32)
    red[2 * g.x + g.c, :, 0:width] = jnp.where(sub == 0, inner[0], jnp.where(sub == 1, inner[1], 0.0))
    slot = red.at[2 * g.x + g.c]
    for d in (0, 1, -1, 2):
        for k in (0, 1):
            if d or k:
                cp.start(("g1", d, k), slot, slot, {"tp": g.at(0, d, k == 1)})
    for h in (0, 1):
        pass_on(h, 2)
    for d in (0, 1, -1, 2):
        for k in (0, 1):
            if d or k:
                c = 1 - g.c if k else g.c
                cp.wait(("g1", d, k), red.at[2 * x_of(-d) + c], {"tp": g.at(0, -d, k == 1)})
    red[8 + g.y] = ((red[0] + red[1]) + (red[2] + red[3])) + ((red[4] + red[5]) + (red[6] + red[7]))
    for d in (1, -1, 2):
        cp.start(("g2", d), red.at[8 + g.y], red.at[8 + g.y], {"tp": g.at(d, 0)})
    for h in (0, 1):
        for o1 in (0, -1, 1, 2):
            landed(h, o1)
    for d in (1, -1, 2):
        cp.wait(("g2", d), red.at[8 + y_of(-d)], {"tp": g.at(-d, 0)})
    gc_ref[...] = ((red[8] + red[9]) + (red[10] + red[11]))[0:2, 0:width]
    cp.finish()


N_COPIES = 2 * 7 + (36 + 32) + (4 + 4 + 8 + 32 + 16 + 16) + 1 + 12 + 6 + 10


def layer(tokens, cotangent, ids, weights, gate_w, up_w, down_w):
    width = tokens.shape[1]
    model, size = gate_w.shape
    n = model // width
    ANY = pl.BlockSpec(memory_space=pl.ANY)
    half_w = width // 2
    return pl.pallas_call(
        layer_kernel,
        out_shape=(
            pltpu.VMEM((3, width, n * size), BF16),
                        pltpu.VMEM((2, *cotangent.shape), BF16),
            pltpu.VMEM(ids.shape, F32),
        ),
        in_specs=[ANY] * 7,
        out_specs=(VMEM,) * 3,
        scratch_shapes=[
            pltpu.VMEM(tokens.shape, BF16),
            pltpu.VMEM(tokens.shape, BF16),
            pltpu.VMEM(ids.shape, jnp.int32),
            pltpu.VMEM(ids.shape, F32),
            pltpu.VMEM((model, size), BF16),
            pltpu.VMEM((model, size), BF16),
            pltpu.VMEM((size, model), BF16),
            pltpu.VMEM((size, model), BF16),
            pltpu.VMEM((size, model), BF16),
            pltpu.VMEM((model, size), BF16),
            pltpu.VMEM((ROWS, PACK), BF16),
            pltpu.VMEM((model, PACK), BF16),
            pltpu.VMEM((2, SIDE * width, WIN), BF16),
            pltpu.VMEM((2, SIDE * width, WIN), BF16),
            pltpu.VMEM((size, WIN), BF16),
            pltpu.VMEM((size, WIN), BF16),
            pltpu.VMEM((size, WIN), BF16),
            pltpu.VMEM((2, SIDE, 2, size // 2, 1024), BF16),
            pltpu.VMEM((2, SIDE, 2, 3, 3, width, size // 2), BF16),
            pltpu.VMEM((2, SIDE, 2, 3, width, size // 2), BF16),
            pltpu.VMEM((2, SIDE * SIDE, width, PACK), BF16),
            pltpu.VMEM((SIDE * SIDE, width, PACK), BF16),
            pltpu.VMEM((SIDE, SIDE, width, PACK), BF16),
            pltpu.VMEM((2, 2, 2, half_w, PACK), BF16),
            pltpu.VMEM((2, 2, 2, half_w, PACK), BF16),
            pltpu.VMEM((2, 2, 2, 2, half_w, PACK), BF16),
            pltpu.VMEM((2, SIDE, half_w, PACK), BF16),
            pltpu.VMEM((2, 3, half_w, PACK), BF16),
            pltpu.VMEM((ROWS, width), BF16),
            pltpu.VMEM((ROWS, width), BF16),
            pltpu.VMEM((ROWS, width), BF16),
            pltpu.VMEM((ROWS, width), BF16),
            pltpu.VMEM((12, 8, 128), F32),
            pltpu.SemaphoreType.DMA((7,)),
            pltpu.SemaphoreType.DMA((N_COPIES,)),
            pltpu.SemaphoreType.DMA((N_COPIES,)),
        ],
        compiler_params=pltpu.CompilerParams(
            collective_id=0, has_side_effects=True, vmem_limit_bytes=52 * 2**20
        ),
        name="layer",
    )(tokens, cotangent, ids, weights, gate_w, up_w, down_w)


def out_kernel(wide, rows, gc, mixed, gt, gco, gate, up, down, sem):
    pairs = ((wide.at[0], gate), (wide.at[1], up), (wide.at[2], down), (rows.at[0], mixed), (rows.at[1], gt), (gc, gco))
    copies = [pltpu.make_async_copy(a, b, sem.at[i]) for i, (a, b) in enumerate(pairs)]
    for c in copies:
        c.start()
    for c in copies:
        c.wait()


def results(wide, rows, gc):
    shapes = [rows.shape[1:]] * 2 + [gc.shape] + [wide.shape[1:]] * 3
    types = [BF16, BF16, F32, BF16, BF16, BF16]
    return pl.pallas_call(
        out_kernel,
        out_shape=tuple(jax.ShapeDtypeStruct(a, t) for a, t in zip(shapes, types)),
        in_specs=[VMEM] * 3,
        out_specs=(pl.BlockSpec(memory_space=pl.ANY),) * 6,
        scratch_shapes=[pltpu.SemaphoreType.DMA((6,))],
        compiler_params=pltpu.CompilerParams(vmem_limit_bytes=8 * 2**20),
        name="results",
    )(wide, rows, gc)


def body(tokens, cotangent, expert_ids, combine_weights, w_gate, w_up, w_down):
    wide, back, gc = layer(
        tokens, cotangent, expert_ids.T, combine_weights.T, w_gate[0], w_up[0], w_down[0]
    )
    mixed, gt, gc, gate, up, down = results(wide, back, gc)
    return mixed, gt, gc.T, gate[None], up[None], down.T[None]


def solution(mesh):
    placed = (
        P("ep", "tp"),
        P("ep", "tp"),
        P("ep", None),
        P("ep", None),
        P("ep", None, "tp"),
        P("ep", None, "tp"),
        P("ep", "tp", None),
    )
    return jax.shard_map(
        body,
        mesh=mesh,
        in_specs=placed,
        out_specs=(
            P("ep", "tp"),
            P("ep", "tp"),
            P("ep", None),
            P("ep", "tp", None),
            P("ep", "tp", None),
            P("ep", None, "tp"),
        ),
        check_vma=False,
    )
```

```python
import jax
import jax.numpy as jnp
from jax import lax
from jax.experimental import pallas as pl
from jax.experimental.pallas import tpu as pltpu
from jax.sharding import PartitionSpec as P

SIDE = 4
CAP = 40
HALF = CAP
PAIR = 2 * HALF
GROUPS = 8
ROWS = GROUPS * PAIR
SLOTS = GROUPS * CAP
PACK = 2 * SLOTS
WIN = 384
F32 = jnp.float32
BF16 = jnp.bfloat16
VMEM = pl.BlockSpec(memory_space=pltpu.VMEM)


def dot(a, b, ca, cb):
    return lax.dot_general(a, b, (((ca,), (cb,)), ((), ())), preferred_element_type=F32)


def iota(shape, dim):
    return lax.broadcasted_iota(jnp.int32, shape, dim)


class Grid:
    def __init__(self):
        t = lax.axis_index("tp")
        self.tp = t
        self.c = t % 2
        self.x = (t // 2) % SIDE
        self.y = t // (2 * SIDE)
        self.z = lax.axis_index("ep")

    def at(self, dy, dx, other=False):
        y = (self.y + (dy + SIDE)) % SIDE
        x = (self.x + (dx + SIDE)) % SIDE
        c = 1 - self.c if other else self.c
        return (y * SIDE + x) * 2 + c

    def block(self, h, o1, o2, other=False):
        return self.at(o2, o1, other) if h == 0 else self.at(o1, o2, other)

    def up(self, k):
        return (self.z + k) % GROUPS


class Copies:
    def __init__(self, send, recv):
        self.send, self.recv, self.n, self.ids, self.started = send, recv, 0, {}, []

    def make(self, key, src, dst, to):
        if key not in self.ids:
            self.ids[key] = len(self.ids)
        j = self.ids[key]
        return pltpu.make_async_remote_copy(
            src_ref=src,
            dst_ref=dst,
            send_sem=self.send.at[j],
            recv_sem=self.recv.at[j],
            device_id=to,
            device_id_type=pl.DeviceIdType.MESH,
        )

    def start(self, key, src, dst, to):
        c = self.make(key, src, dst, to)
        c.start()
        self.started.append(c)

    def wait(self, key, dst, to):
        self.make(key, dst, dst, to).wait_recv()

    def finish(self):
        for c in self.started:
            c.wait_send()


def greet(partners):
    barrier = pltpu.get_barrier_semaphore()
    for to in partners:
        pl.semaphore_signal(barrier, inc=1, device_id=to, device_id_type=pl.DeviceIdType.MESH)


def greeted(partners):
    pl.semaphore_wait(pltpu.get_barrier_semaphore(), len(partners))


def gather(g, cp, name, half, part):
    sib = {"tp": g.at(0, 0, True)}
    dirs = (1, -1)

    def nbr(h, axis, d):
        return {"tp": g.block(h, d, 0) if axis == 1 else g.block(h, 0, d)}

    def send(key, h, axis, d, ref):
        cp.start((name, *key), ref, ref, nbr(h, axis, d))

    def got(key, h, axis, d, ref):
        cp.wait((name, *key), ref, nbr(h, axis, d))

    def across(h, o1, o2):
        ref = half(g.block(h, o1, o2), h)
        cp.start((name, "s", h, o1, o2), ref, ref, sib)

    for h in (0, 1):
        for d in dirs + (2,):
            send(("p1", h, d), h, 1, d, half(g.tp, h))
    for h in (0, 1):
        for d in dirs:
            send(("p2", h, 0, d), h, 2, d, half(g.tp, h))
    for h in (0, 1):
        across(h, 0, 0)
    for d in dirs:
        for h in (0, 1):
            b = g.block(h, -d, 0)
            got(("p1", h, d), h, 1, -d, half(b, h))
            for e in dirs:
                send(("p2", h, -d, e), h, 2, e, half(b, h))
            across(h, -d, 0)
    for h in (0, 1):
        b = g.block(h, 2, 0)
        got(("p1", h, 2), h, 1, 2, half(b, h))
        for e in dirs + (2,):
            send(("p2", h, 2, e), h, 2, e, half(b, h))
        across(h, 2, 0)
    for e in dirs:
        for h in (0, 1):
            b = g.block(h, 0, -e)
            got(("p2", h, 0, e), h, 2, -e, half(b, h))
            send(("f2", h, 0, e), h, 2, e, part(b, h, e, 0))
            across(h, 0, -e)
    for o1 in (-1, 1):
        for e in dirs:
            for h in (0, 1):
                b = g.block(h, o1, -e)
                got(("p2", h, o1, e), h, 2, -e, half(b, h))
                send(("f2", h, o1, e), h, 2, e, part(b, h, e, o1))
                across(h, o1, -e)
    for h in (0, 1):
        b = g.block(h, 0, 2)
        for e in dirs:
            got(("f2", h, 0, e), h, 2, -e, part(b, h, e, 0))
        across(h, 0, 2)
    for e in dirs:
        for h in (0, 1):
            b = g.block(h, 2, -e)
            got(("p2", h, 2, e), h, 2, -e, half(b, h))
            across(h, 2, -e)
    for o1 in (-1, 1):
        for h in (0, 1):
            b = g.block(h, o1, 2)
            for e in dirs:
                got(("f2", h, o1, e), h, 2, -e, part(b, h, e, o1))
            across(h, o1, 2)
    for h in (0, 1):
        b = g.block(h, 2, 2)
        got(("p2", h, 2, 2), h, 2, 2, half(b, h))
        across(h, 2, 2)
    for h in (0, 1):
        for o1 in (0, -1, 1, 2):
            for o2 in (0, -1, 1, 2):
                cp.wait((name, "s", h, o1, o2), half(g.block(h, o1, o2, True), h), sib)


def column(row):
    n = row.shape[1]
    eye = iota((n, n), 0) == iota((n, n), 1)
    return jnp.sum(jnp.where(eye, row, jnp.zeros_like(row)), axis=1, keepdims=True)


def as_row(col):
    n = col.shape[0]
    eye = iota((n, n), 0) == iota((n, n), 1)
    return jnp.sum(jnp.where(eye, col, jnp.zeros_like(col)), axis=0, keepdims=True)


def places(ids):
    n = ids[0].shape[0]
    lane = iota((n, 128), 1).astype(F32)
    before = (iota((n, n), 1) < iota((n, n), 0)).astype(BF16)
    hot = [(ids[k] == lane).astype(F32) for k in (0, 1)]
    seen = [dot(before, hot[k].astype(BF16), 1, 0) for k in (0, 1)]
    seen[1] = seen[1] + jnp.sum(hot[0], axis=0, keepdims=True)
    rank = [jnp.sum(seen[k] * hot[k], axis=1, keepdims=True) for k in (0, 1)]
    row = [ids[k] * PAIR + rank[k] for k in (0, 1)]
    lanes = iota((n, ROWS), 1).astype(F32)
    first = [(lanes == row[k]).astype(BF16) for k in (0, 1)]
    second = [(lanes == row[k] + HALF).astype(BF16) for k in (0, 1)]
    return first, second


def fill_packing(pack):
    j = iota((PAIR, 1), 0)
    lane = iota((PAIR, PACK), 1)
    for z in range(GROUPS):
        s = z * CAP + j
        d = s - CAP
        want = jnp.where(j >= CAP, jnp.where(d < 256, d + 384, d + 64), s)
        pack[z * PAIR : (z + 1) * PAIR, :] = (want == lane).astype(F32).astype(BF16)


def to_all_groups(g, cp, src, dst, name):
    for k in range(1, GROUPS):
        to = g.up(k)
        cp.start(
            (name, k),
            src.at[pl.ds(pl.multiple_of(to * PAIR, PAIR), PAIR)],
            dst.at[pl.ds(pl.multiple_of(g.z * PAIR, PAIR), PAIR)],
            {"ep": to},
        )


def from_all_groups(g, cp, dst, name):
    for k in range(1, GROUPS):
        frm = g.up(GROUPS - k)
        cp.wait((name, k), dst.at[pl.ds(pl.multiple_of(frm * PAIR, PAIR), PAIR)], {"ep": frm})


def own_group(g, src, dst):
    mine = pl.ds(pl.multiple_of(g.z * PAIR, PAIR), PAIR)
    dst[mine] = src[mine]


def turned(t):
    return pltpu.roll(t, 64, 1)


def layer_kernel(
    tok_hbm, cot_hbm, ids_hbm, w_hbm, gw_hbm, uw_hbm, dw_hbm,
    wide_ref, rows_ref, gc_ref,
    tok_ref, cot_ref, ids_ref, w_ref,
    gw, uw, dw, gwt, uwt, dwt, pack, all_ref, wx, wd, hx, gy, uy,
    act, ship, relay, part_ref, sib, chip, far, tmp, near, mid, fin,
    rows, got, rows2, got2, red, local, send, recv,
):
    g = Grid()
    cp = Copies(send, recv)
    sib_dev = {"tp": g.at(0, 0, True)}
    ring = ((0, 1), (0, -1), (0, 2), (1, 0), (-1, 0), (2, 0))
    others = ((0, 1, True), (0, -1, True), (0, 2, True))
    partners = (
        [sib_dev] + [{"tp": g.at(*o)} for o in ring + others] + [{"ep": g.up(k)} for k in range(1, GROUPS)]
    )
    greet(partners)
    loads = [
        pltpu.make_async_copy(a, b, local.at[i])
        for i, (a, b) in enumerate(
            (
                (tok_hbm, tok_ref),
                (cot_hbm, cot_ref),
                (ids_hbm, ids_ref),
                (w_hbm, w_ref),
                (gw_hbm, gw),
                (uw_hbm, uw),
                (dw_hbm, dw),
            )
        )
    ]
    for c in loads:
        c.start()
    for c in loads[:4]:
        c.wait()

    width = tok_ref.shape[1]
    ids = [column(ids_ref[k : k + 1, :].astype(F32)) for k in (0, 1)]
    w = [column(w_ref[k : k + 1, :]) for k in (0, 1)]
    first, second = places(ids)
    cot = cot_ref[...].astype(F32)
    scaled = [(w[k] * cot).astype(BF16) for k in (0, 1)]
    sent = dot(first[0] + first[1], tok_ref[...], 0, 0)
    sent = sent + dot(second[0], scaled[0], 0, 0) + dot(second[1], scaled[1], 0, 0)
    rows[...] = sent.astype(BF16)
    greeted(partners)
    to_all_groups(g, cp, rows, got, "out")
    own_group(g, rows, got)
    fill_packing(pack)
    for c in loads[4:]:
        c.wait()
    size = gw.shape[1]
    blocks = gw.shape[0] // width

    def turn(i, _):
        at = pl.ds(pl.multiple_of(i * 256, 256), 256)
        gwt[:, at] = gw[at, :].T
        uwt[:, at] = uw[at, :].T
        dwt[at, :] = dw[:, at].T
        return _

    lax.fori_loop(0, gw.shape[0] // 256, turn, 0)
    from_all_groups(g, cp, got, "out")
    own = dot(got[...], pack[...], 0, 0).astype(BF16)
    all_ref[pl.ds(pl.multiple_of(g.tp * width, width), width), :] = own
    half_w = width // 2

    def half_in(b, h):
        return all_ref.at[pl.ds(pl.multiple_of(b * width + h * half_w, 16), half_w)]

    def part_in(b, h, q, o):
        rng = pl.ds(0, 384) if (q > 0) == (o in (0, 1)) else pl.ds(384, 256)
        return all_ref.at[pl.ds(pl.multiple_of(b * width + h * half_w, 16), half_w), rng]

    gather(g, cp, "in", half_in, part_in)

    hh = size // 2

    def units(h, _):
        r = pl.ds(h * hh, hh)
        gate = dot(gwt[r, :], all_ref[:, :WIN], 1, 0)
        upp = dot(uwt[r, :], all_ref[:, :WIN], 1, 0)
        gh = dot(dw[r, :], all_ref[:, 256:], 1, 0)
        place = g.x if h == 0 else g.y
        lo = iota((hh, 128), 1) < 64
        for i in range(3):
            t = slice(i * 128, (i + 1) * 128)
            gp, u = gate[:, t], upp[:, t]
            d = turned(gh[:, 0:128]) if i == 2 else gh[:, (i + 1) * 128 : (i + 2) * 128]
            s = jax.nn.sigmoid(gp)
            active = gp * s
            hid = active * u
            gg = d * u * (s * (1.0 + gp * (1.0 - s)))
            gu = d * active
            if i == 2:
                hid, gg, gu = (jnp.where(lo, a, 0.0) for a in (hid, gg, gu))
                act[h, place, g.c, :, 256:384] = (gg + turned(hid)).astype(BF16)
                gy[r, 0:128] = turned(gg).astype(BF16)
                uy[r, 0:128] = turned(gu).astype(BF16)
            else:
                act[h, place, g.c, :, t] = gg.astype(BF16)
                act[h, place, g.c, :, 384 + i * 128 : 512 + i * 128] = hid.astype(BF16)
                gy[r, (i + 1) * 128 : (i + 2) * 128] = gg.astype(BF16)
                uy[r, (i + 1) * 128 : (i + 2) * 128] = gu.astype(BF16)
            hx[r, t] = hid.astype(BF16)
            act[h, place, g.c, :, 640 + i * 128 : 768 + i * 128] = gu.astype(BF16)
        return _


    dirs = (1, -1)
    dests = (0, 1, -1, 2)
    lines = (0, -1, 1, 2)

    def spot(h, o1):
        return ((g.x if h == 0 else g.y) + (o1 + SIDE)) % SIDE

    def nbr(h, axis, d):
        return {"tp": g.block(h, d, 0) if axis == 1 else g.block(h, 0, d)}

    def piece(h, o1, d):
        return act.at[h, spot(h, o1), g.c, pl.ds(0 if d > 0 else hh // 2, hh // 2)]

    def cross(h, o1):
        ref = act.at[h, spot(h, o1), g.c]
        cp.start(("s", h, o1), ref, ref, sib_dev)

    def crossed(h, o1):
        cp.wait(("s", h, o1), act.at[h, spot(h, o1), 1 - g.c], sib_dev)

    def columns(h, o1, o2, k):
        b = g.block(h, o1, o2, k == 1)
        return pl.ds(pl.multiple_of(b * size + h * hh, 128), hh)

    def make(h, o1, k):
        j = lines.index(o1)
        c = g.c if k == 0 else 1 - g.c
        blk = act[h, spot(h, o1), c]
        for i, (left, right) in enumerate(
            ((wx[h], blk[:, :WIN]), (wx[h], blk[:, 640:]), (wd[h], blk[:, 256:640]))
        ):
            res = dot(left, right, 1, 1).astype(BF16)
            wide_ref[i, :, columns(h, o1, 0, k)] = res[0:width]
            for n in range(3):
                ship[h, j, k, n, i] = res[(n + 1) * width : (n + 2) * width]
        for n, d in enumerate(dirs):
            cp.start(
                ("w", h, o1, k, d), ship.at[h, j, k, n], wide_ref.at[:, :, columns(h, o1, 0, k)], nbr(h, 2, d)
            )
        d = dirs[k]
        cp.start(("v", h, o1, d), ship.at[h, j, k, 2], relay.at[h, j, k], nbr(h, 2, d))

    def pass_on(h, o1):
        j = lines.index(o1)
        for k, d in enumerate(dirs):
            cp.wait(("v", h, o1, d), relay.at[h, j, k], nbr(h, 2, -d))
            cp.start(
                ("u", h, o1, d), relay.at[h, j, k], wide_ref.at[:, :, columns(h, o1, -d, k)], nbr(h, 2, d)
            )

    def landed(h, o1):
        for k, d in enumerate(dirs):
            for e in dirs:
                cp.wait(("w", h, o1, k, e), wide_ref.at[:, :, columns(h, o1, -e, k)], nbr(h, 2, -e))
            cp.wait(("u", h, o1, d), wide_ref.at[:, :, columns(h, o1, 2, k)], nbr(h, 2, -d))

    for h in (0, 1):
        units(h, 0)
        ref = act.at[h, spot(h, 0), g.c]
        for d in dirs:
            cp.start(("p", h, d), ref, ref, nbr(h, 1, d))
        cross(h, 0)
    low = iota((width, 128), 1) < 64
    for h in (0, 1):
        for n, o2 in enumerate(dests):
            at = pl.ds(pl.multiple_of(g.block(h, 0, o2) * width, width), width)
            r = pl.ds(n * width, width)
            shared = all_ref[at, 256:384].astype(F32)
            wx[h, r, 0:256] = all_ref[at, 0:256]
            wx[h, r, 256:384] = jnp.where(low, shared, 0.0).astype(BF16)
            wd[h, r, 0:128] = jnp.where(low, 0.0, shared).astype(BF16)
            wd[h, r, 128:384] = all_ref[at, 384:640]
    for h in (0, 1):
        make(h, 0, 0)
    for h in (0, 1):
        crossed(h, 0)
        make(h, 0, 1)

    def partial(c):
        def one(i, _):
            at = pl.ds(pl.multiple_of((2 * i + c) * width, width), width)
            out = dot(dwt[at, :], hx[...], 1, 0)
            inn = dot(gw[at, :], gy[...], 1, 0) + dot(uw[at, :], uy[...], 1, 0)
            part_ref[c, i, :, 0:256] = out[:, 0:256].astype(BF16)
            part_ref[c, i, :, 256:384] = (out[:, 256:] + inn[:, :128]).astype(BF16)
            part_ref[c, i, :, 384:640] = inn[:, 128:].astype(BF16)
            return _

        lax.fori_loop(0, blocks // 2, one, 0)

    partial(1 - g.c)
    cp.start("pair", part_ref.at[1 - g.c], sib, sib_dev)
    partial(g.c)
    for d in dirs:
        for h in (0, 1):
            cp.wait(("p", h, d), act.at[h, spot(h, -d), g.c], nbr(h, 1, -d))
            cp.start(("f", h, d), piece(h, -d, d), piece(h, -d, d), nbr(h, 1, d))
            cross(h, -d)
    cp.wait("pair", sib, sib_dev)

    def add_pair(i, _):
        chip[i // SIDE, i % SIDE] = (part_ref[g.c, i].astype(F32) + sib[i].astype(F32)).astype(BF16)
        return _

    lax.fori_loop(0, SIDE * SIDE, add_pair, 0)

    def y_of(d):
        return (g.y + d + SIDE) % SIDE

    def x_of(d):
        return (g.x + d + SIDE) % SIDE

    rng = (pl.ds(0, half_w), pl.ds(half_w, half_w))

    def share(h, d, q):
        two = pl.ds(2 * q, 2)
        return (y_of(d), two, rng[0]) if h == 0 else (two, x_of(d), rng[1])

    for h in (0, 1):
        for q, d in enumerate(dirs):
            cp.start(("r1", h, d), chip.at[share(h, 2, q)], far.at[h, q], nbr(h, 2, d))
        for q, d in enumerate(dirs):
            cp.start(("r2", h, d), chip.at[share(h, d, 1 - q)], near.at[h, q, 1], nbr(h, 2, d))
    for q, d in enumerate(dirs):
        for h in (0, 1):
            cp.wait(("r1", h, d), far.at[h, q], nbr(h, 2, -d))
            tmp[h, q] = (chip[share(h, d, q)].astype(F32) + far[h, q].astype(F32)).astype(BF16)
            cp.start(("r3", h, d), tmp.at[h, q], near.at[h, q, 0], nbr(h, 2, d))
    for h in (0, 1):
        pass_on(h, 0)
    for d in dirs:
        for h in (0, 1):
            make(h, -d, 0)
    for h in (0, 1):
        for q, d in enumerate(dirs):
            cp.wait(("r2", h, d), near.at[h, q, 1], nbr(h, 2, -d))
            cp.wait(("r3", h, d), near.at[h, q, 0], nbr(h, 2, -d))
        for q in (0, 1):
            t = chip[share(h, 0, q)].astype(F32)
            t = t + near[h, q, 0].astype(F32) + near[h, 1 - q, 1].astype(F32)
            mid[h, 2 * q : 2 * q + 2] = t.astype(BF16)
    for i, d in enumerate((1, -1, 2)):
        cp.start(("a2", d), mid.at[0, x_of(d)], fin.at[0, i], {"tp": g.at(0, d)})
        cp.start(("b2", d), mid.at[1, y_of(d)], fin.at[1, i], {"tp": g.at(d, 0)})
    for d in dirs:
        for h in (0, 1):
            crossed(h, -d)
            make(h, -d, 1)
    for h in (0, 1):
        for d in dirs:
            cp.wait(("f", h, d), piece(h, 2, d), nbr(h, 1, -d))
        cross(h, 2)
        make(h, 2, 0)
    for h in (0, 1):
        crossed(h, 2)
        make(h, 2, 1)
    for i, d in enumerate((1, -1, 2)):
        cp.wait(("a2", d), fin.at[0, i], {"tp": g.at(0, -d)})
        cp.wait(("b2", d), fin.at[1, i], {"tp": g.at(-d, 0)})
    sums = []
    for h in (0, 1):
        s = mid[h, g.x if h == 0 else g.y].astype(F32)
        for i in range(3):
            s = s + fin[h, i].astype(F32)
        sums.append(s)
    total = jnp.concatenate(sums, axis=0).astype(BF16)
    rows2[...] = dot(pack[...], total, 1, 1).astype(BF16)
    to_all_groups(g, cp, rows2, got2, "back")
    own_group(g, rows2, got2)
    for h in (0, 1):
        for o1 in (-1, 1):
            pass_on(h, o1)
    from_all_groups(g, cp, got2, "back")
    back = got2[...]
    outs = [dot(first[k], back, 1, 0) for k in (0, 1)]
    rows_ref[0] = (w[0] * outs[0] + w[1] * outs[1]).astype(BF16)
    rows_ref[1] = (dot(second[0], back, 1, 0) + dot(second[1], back, 1, 0)).astype(BF16)
    inner = [as_row(jnp.sum(cot * outs[k], axis=1, keepdims=True)) for k in (0, 1)]
    sub = iota((8, width), 0)
    red[2 * g.x + g.c] = jnp.zeros((8, 128), F32)
    red[2 * g.x + g.c, :, 0:width] = jnp.where(sub == 0, inner[0], jnp.where(sub == 1, inner[1], 0.0))
    slot = red.at[2 * g.x + g.c]
    for d in (0, 1, -1, 2):
        for k in (0, 1):
            if d or k:
                cp.start(("g1", d, k), slot, slot, {"tp": g.at(0, d, k == 1)})
    for h in (0, 1):
        pass_on(h, 2)
    for d in (0, 1, -1, 2):
        for k in (0, 1):
            if d or k:
                c = 1 - g.c if k else g.c
                cp.wait(("g1", d, k), red.at[2 * x_of(-d) + c], {"tp": g.at(0, -d, k == 1)})
    red[8 + g.y] = ((red[0] + red[1]) + (red[2] + red[3])) + ((red[4] + red[5]) + (red[6] + red[7]))
    for d in (1, -1, 2):
        cp.start(("g2", d), red.at[8 + g.y], red.at[8 + g.y], {"tp": g.at(d, 0)})
    for h in (0, 1):
        for o1 in (0, -1, 1, 2):
            landed(h, o1)
    for d in (1, -1, 2):
        cp.wait(("g2", d), red.at[8 + y_of(-d)], {"tp": g.at(-d, 0)})
    gc_ref[...] = ((red[8] + red[9]) + (red[10] + red[11]))[0:2, 0:width]
    cp.finish()


N_COPIES = 2 * 7 + (36 + 32) + (4 + 4 + 8 + 32 + 16 + 16) + 1 + 12 + 6 + 10


def layer(tokens, cotangent, ids, weights, gate_w, up_w, down_w):
    width = tokens.shape[1]
    model, size = gate_w.shape
    n = model // width
    ANY = pl.BlockSpec(memory_space=pl.ANY)
    half_w = width // 2
    return pl.pallas_call(
        layer_kernel,
        out_shape=(
            pltpu.VMEM((3, width, n * size), BF16),
                        pltpu.VMEM((2, *cotangent.shape), BF16),
            pltpu.VMEM(ids.shape, F32),
        ),
        in_specs=[ANY] * 7,
        out_specs=(VMEM,) * 3,
        scratch_shapes=[
            pltpu.VMEM(tokens.shape, BF16),
            pltpu.VMEM(tokens.shape, BF16),
            pltpu.VMEM(ids.shape, jnp.int32),
            pltpu.VMEM(ids.shape, F32),
            pltpu.VMEM((model, size), BF16),
            pltpu.VMEM((model, size), BF16),
            pltpu.VMEM((size, model), BF16),
            pltpu.VMEM((size, model), BF16),
            pltpu.VMEM((size, model), BF16),
            pltpu.VMEM((model, size), BF16),
            pltpu.VMEM((ROWS, PACK), BF16),
            pltpu.VMEM((model, PACK), BF16),
            pltpu.VMEM((2, SIDE * width, WIN), BF16),
            pltpu.VMEM((2, SIDE * width, WIN), BF16),
            pltpu.VMEM((size, WIN), BF16),
            pltpu.VMEM((size, WIN), BF16),
            pltpu.VMEM((size, WIN), BF16),
            pltpu.VMEM((2, SIDE, 2, size // 2, 1024), BF16),
            pltpu.VMEM((2, SIDE, 2, 3, 3, width, size // 2), BF16),
            pltpu.VMEM((2, SIDE, 2, 3, width, size // 2), BF16),
            pltpu.VMEM((2, SIDE * SIDE, width, PACK), BF16),
            pltpu.VMEM((SIDE * SIDE, width, PACK), BF16),
            pltpu.VMEM((SIDE, SIDE, width, PACK), BF16),
            pltpu.VMEM((2, 2, 2, half_w, PACK), BF16),
            pltpu.VMEM((2, 2, 2, half_w, PACK), BF16),
            pltpu.VMEM((2, 2, 2, 2, half_w, PACK), BF16),
            pltpu.VMEM((2, SIDE, half_w, PACK), BF16),
            pltpu.VMEM((2, 3, half_w, PACK), BF16),
            pltpu.VMEM((ROWS, width), BF16),
            pltpu.VMEM((ROWS, width), BF16),
            pltpu.VMEM((ROWS, width), BF16),
            pltpu.VMEM((ROWS, width), BF16),
            pltpu.VMEM((12, 8, 128), F32),
            pltpu.SemaphoreType.DMA((7,)),
            pltpu.SemaphoreType.DMA((N_COPIES,)),
            pltpu.SemaphoreType.DMA((N_COPIES,)),
        ],
        compiler_params=pltpu.CompilerParams(
            collective_id=0, has_side_effects=True, vmem_limit_bytes=52 * 2**20
        ),
        name="layer",
    )(tokens, cotangent, ids, weights, gate_w, up_w, down_w)


def out_kernel(wide, rows, gc, mixed, gt, gco, gate, up, down, sem):
    pairs = ((wide.at[0], gate), (wide.at[1], up), (wide.at[2], down), (rows.at[0], mixed), (rows.at[1], gt), (gc, gco))
    copies = [pltpu.make_async_copy(a, b, sem.at[i]) for i, (a, b) in enumerate(pairs)]
    for c in copies:
        c.start()
    for c in copies:
        c.wait()


def results(wide, rows, gc):
    shapes = [rows.shape[1:]] * 2 + [gc.shape] + [wide.shape[1:]] * 3
    types = [BF16, BF16, F32, BF16, BF16, BF16]
    return pl.pallas_call(
        out_kernel,
        out_shape=tuple(jax.ShapeDtypeStruct(a, t) for a, t in zip(shapes, types)),
        in_specs=[VMEM] * 3,
        out_specs=(pl.BlockSpec(memory_space=pl.ANY),) * 6,
        scratch_shapes=[pltpu.SemaphoreType.DMA((6,))],
        compiler_params=pltpu.CompilerParams(vmem_limit_bytes=8 * 2**20),
        name="results",
    )(wide, rows, gc)


def body(tokens, cotangent, expert_ids, combine_weights, w_gate, w_up, w_down):
    wide, back, gc = layer(
        tokens, cotangent, expert_ids.T, combine_weights.T, w_gate[0], w_up[0], w_down[0]
    )
    mixed, gt, gc, gate, up, down = results(wide, back, gc)
    return mixed, gt, gc.T, gate[None], up[None], down.T[None]


def solution(mesh):
    placed = (
        P("ep", "tp"),
        P("ep", "tp"),
        P("ep", None),
        P("ep", None),
        P("ep", None, "tp"),
        P("ep", None, "tp"),
        P("ep", "tp", None),
    )
    return jax.shard_map(
        body,
        mesh=mesh,
        in_specs=placed,
        out_specs=(
            P("ep", "tp"),
            P("ep", "tp"),
            P("ep", None),
            P("ep", "tp", None),
            P("ep", "tp", None),
            P("ep", None, "tp"),
        ),
        check_vma=False,
    )
```
